32 devices in a mesh: layer: 1 (over z), tensor: 32 (over y, x, core).
Axes of the slice: x: 4, y: 4, z: 1, core: 2. Of those that a mesh axis runs over, the one named last changes fastest.
The devices are a block of a 4x4x8 slice.
Arguments:
- gradient: bfloat16 [4096, 4096], P('layer', 'tensor')
- left_stat: float32 [4096, 4096], P('layer')
- right_stat: float32 [4096, 1024], P(('layer', 'tensor'))
- left_root: bfloat16 [4096, 4096], P('layer')
- right_root: bfloat16 [4096, 1024], P(('layer', 'tensor'))
Outputs:
- output 1: float32 [4096, 4096], P('layer')
- output 2: float32 [4096, 1024], P(('layer', 'tensor'))
- output 3: float32 [4096, 4096], P('layer', 'tensor')
All inputs are finite; a program needn't handle non-finite values.
Results may differ from the reference program's by a relative error of at most 0.001.
Values are sent between devices in bfloat16 or wider.
A program may use at most 768 MiB of HBM per device.

```python
import jax
import jax.numpy as jnp

GRAD_ROWS = 4096
GRAD_COLS = 4096
BLOCK_SIZE = 1024
EMA_DECAY = 0.9


def setup_inputs(seed: int = 0, part: int = 0) -> dict:
    base_key = jax.random.fold_in(jax.random.key(seed), part)
    key_list = jax.random.split(base_key, 8)
    low_rank = 32
    num_blocks = GRAD_COLS // BLOCK_SIZE
    grad_scale = (GRAD_ROWS * GRAD_COLS) ** -0.25
    left_scale = (GRAD_COLS / GRAD_ROWS) ** 0.5
    right_scale = (GRAD_ROWS / GRAD_COLS) ** 0.5
    grad_noise = jax.random.normal(key_list[0], (GRAD_ROWS, GRAD_COLS), jnp.float32)
    row_factor = jax.random.normal(key_list[1], (GRAD_ROWS, low_rank), jnp.float32)
    col_factor = jax.random.normal(key_list[2], (GRAD_COLS, low_rank), jnp.float32)
    shared = jnp.dot(row_factor, col_factor.T) * low_rank ** -0.5
    gradient = ((grad_noise + shared) * (grad_scale * 0.5 ** 0.5)).astype(jnp.bfloat16)
    left_noise = jax.random.normal(key_list[3], (GRAD_ROWS, GRAD_ROWS), jnp.float32)
    left_stat = (left_scale / 9.0) * (jnp.eye(GRAD_ROWS, dtype=jnp.float32) + 0.1 * (left_noise + left_noise.T))
    diag_mask = (jnp.arange(GRAD_COLS)[:, None] % BLOCK_SIZE == jnp.arange(BLOCK_SIZE)[None, :]).astype(jnp.float32)
    right_noise = jax.random.normal(key_list[4], (GRAD_COLS, BLOCK_SIZE), jnp.float32)
    right_stat = (right_scale / 9.0) * (diag_mask + 0.15 * right_noise)
    left_fac = jax.random.normal(key_list[5], (GRAD_ROWS, low_rank), jnp.float32)
    left_sq = jnp.dot(left_fac, left_fac.T) * (GRAD_ROWS * low_rank) ** -0.5
    left_root = (GRAD_ROWS ** 0.25 * (0.5 * jnp.eye(GRAD_ROWS, dtype=jnp.float32) + left_sq)).astype(jnp.bfloat16)
    right_fac = jax.random.normal(key_list[6], (num_blocks, BLOCK_SIZE, low_rank), jnp.float32)
    right_sq = jnp.einsum('cir,cjr->cij', right_fac, right_fac) * (BLOCK_SIZE * low_rank) ** -0.5
    right_sym = 0.5 * (right_sq + jnp.swapaxes(right_sq, 1, 2)) + 0.5 * jnp.eye(BLOCK_SIZE, dtype=jnp.float32)
    right_root = (GRAD_COLS ** 0.25 * right_sym).reshape(GRAD_COLS, BLOCK_SIZE).astype(jnp.bfloat16)
    return {'gradient': gradient, 'left_stat': left_stat, 'right_stat': right_stat, 'left_root': left_root, 'right_root': right_root}


def reference(gradient, left_stat, right_stat, left_root, right_root):
    num_blocks = GRAD_COLS // BLOCK_SIZE
    left_prod = jnp.dot(gradient, gradient.T, preferred_element_type=jnp.float32)
    left_new = EMA_DECAY * left_stat + (1.0 - EMA_DECAY) * left_prod
    grad_blocks = gradient.astype(jnp.float32).reshape(GRAD_ROWS, num_blocks, BLOCK_SIZE)
    right_prod = jnp.einsum('mci,mcj->cij', grad_blocks, grad_blocks)
    right_new = EMA_DECAY * right_stat + (1.0 - EMA_DECAY) * right_prod.reshape(GRAD_COLS, BLOCK_SIZE)
    root_blocks = right_root.astype(jnp.float32).reshape(num_blocks, BLOCK_SIZE, BLOCK_SIZE)
    precond = jnp.einsum('mci,cij->mcj', grad_blocks, root_blocks).astype(jnp.bfloat16)
    precond = precond.reshape(GRAD_ROWS, GRAD_COLS)
    direction = jnp.dot(left_root, precond, preferred_element_type=jnp.float32)
    return (left_new, right_new, direction)
```

```python
import functools

import jax
import jax.numpy as jnp
from jax import lax
from jax.experimental import pallas as pl
from jax.experimental.pallas import tpu as pltpu
from jax.sharding import PartitionSpec as P


EMA_DECAY = 0.9
ROW_PARTS = (2, 2, 2, 1, 1)
TILE = 256
SLABS_PER_DOT = 8
NT = (((1,), (1,)), ((), ()))
TN = (((0,), (0,)), ((), ()))
ANY = pl.BlockSpec(memory_space=pltpu.HBM)


def left_kernel(index, sizes, aliased, *refs):
    chunk_refs = refs[: index + 1]
    refs = refs[index + 1:]
    left_ref = refs[0]
    out_ref = refs[2 if aliased else 1]
    rows_buf, cols_buf, acc, left_a, left_b, out_a, out_b, row_sem, col_sem, la_sem, lb_sem, oa_sem, ob_sem = refs[
        3 if aliased else 2:]
    height = sizes[index]
    base = sum(sizes[:index])
    n_slabs = rows_buf.shape[0]
    n_off = base // TILE
    n_diag = height // TILE
    total = n_off + n_diag

    def load_rows():
        return pltpu.make_async_copy(chunk_refs[index], rows_buf, row_sem)

    def col_copy(k, start, slot):
        return pltpu.make_async_copy(chunk_refs[k].at[:, pl.ds(start, TILE), :], cols_buf.at[slot], col_sem.at[slot])

    def a_in(tile, slot):
        return pltpu.make_async_copy(
            left_ref.at[pl.ds(base, height), pl.ds(pl.multiple_of(tile * TILE, TILE), TILE)], left_a.at[slot], la_sem.at[slot])

    def b_in(tile, slot):
        return pltpu.make_async_copy(
            left_ref.at[pl.ds(pl.multiple_of(tile * TILE, TILE), TILE), pl.ds(base, height)], left_b.at[slot], lb_sem.at[slot])

    def a_out(tile, slot):
        return pltpu.make_async_copy(
            out_a.at[slot], out_ref.at[pl.ds(base, height), pl.ds(pl.multiple_of(tile * TILE, TILE), TILE)], oa_sem.at[slot])

    def b_out(tile, slot):
        return pltpu.make_async_copy(
            out_b.at[slot], out_ref.at[pl.ds(pl.multiple_of(tile * TILE, TILE), TILE), pl.ds(base, height)], ob_sem.at[slot])

    def fetch(step, slot):
        @pl.when(step < n_diag)
        def _():
            a_in(n_off + step, slot).start()

        if n_off:
            @pl.when(step >= n_diag)
            def _():
                tile = step - n_diag
                a_in(tile, slot).start()
                b_in(tile, slot).start()
                first = 0
                for k in range(index):
                    count = sizes[k] // TILE

                    @pl.when(jnp.logical_and(tile >= first, tile < first + count))
                    def _(k=k, first=first):
                        col_copy(k, pl.multiple_of((tile - first) * TILE, TILE), slot).start()

                    first += count

    def product(load_cols):
        def piece(kk, _):
            lhs = jnp.concatenate([rows_buf[kk * SLABS_PER_DOT + j] for j in range(SLABS_PER_DOT)], axis=1)
            rhs = jnp.concatenate([load_cols(kk * SLABS_PER_DOT + j) for j in range(SLABS_PER_DOT)], axis=1)
            part = lax.dot_general(lhs, rhs, NT, preferred_element_type=jnp.float32)

            @pl.when(kk == 0)
            def _():
                acc[...] = part

            @pl.when(kk > 0)
            def _():
                acc[...] = acc[...] + part

            return 0

        lax.fori_loop(0, n_slabs // SLABS_PER_DOT, piece, 0)

    load_rows().start()
    fetch(0, 0)
    load_rows().wait()

    def diag(step, _):
        slot = lax.rem(step, 2)
        a_in(0, slot).wait()

        @pl.when(step + 1 < total)
        def _():
            fetch(step + 1, 1 - slot)

        start = pl.multiple_of(step * TILE, TILE)
        product(lambda j: rows_buf[j, pl.ds(start, TILE), :])

        @pl.when(step >= 2)
        def _():
            a_out(0, slot).wait()

        out_a[slot] = EMA_DECAY * left_a[slot] + (1.0 - EMA_DECAY) * acc[...]
        a_out(n_off + step, slot).start()
        return 0

    lax.fori_loop(0, n_diag, diag, 0)

    if n_off:
        def off(tile, _):
            step = tile + n_diag
            slot = lax.rem(step, 2)
            a_in(0, slot).wait()
            b_in(0, slot).wait()
            col_copy(0, 0, slot).wait()

            @pl.when(step + 1 < total)
            def _():
                fetch(step + 1, 1 - slot)

            product(lambda j: cols_buf[slot, j])

            @pl.when(step >= 2)
            def _():
                a_out(0, slot).wait()

            @pl.when(tile >= 2)
            def _():
                b_out(0, slot).wait()

            out_a[slot] = EMA_DECAY * left_a[slot] + (1.0 - EMA_DECAY) * acc[...]
            out_b[slot] = EMA_DECAY * left_b[slot] + (1.0 - EMA_DECAY) * acc[...].T
            a_out(tile, slot).start()
            b_out(tile, slot).start()
            return 0

        lax.fori_loop(0, n_off, off, 0)
        for slot in range(min(n_off, 2)):
            b_out(0, slot).wait()
    for slot in range(min(total, 2)):
        a_out(0, slot).wait()


def left_update(index, sizes, chunks, left, partial_out):
    height = sizes[index]
    n_slabs, _, width = chunks[0].shape
    aliased = partial_out is not None
    operands = list(chunks) + [left] + ([partial_out] if aliased else [])
    done = sum(sizes[:index])
    area = height * height + 2 * height * done
    return pl.pallas_call(
        functools.partial(left_kernel, index, sizes, aliased),
        out_shape=jax.ShapeDtypeStruct(left.shape, left.dtype),
        in_specs=[ANY] * len(operands),
        out_specs=ANY,
        input_output_aliases={len(operands) - 1: 0} if aliased else {},
        scratch_shapes=[
            pltpu.VMEM((n_slabs, height, width), chunks[0].dtype),
            pltpu.VMEM((2, n_slabs, TILE, width), chunks[0].dtype),
            pltpu.VMEM((height, TILE), jnp.float32),
            pltpu.VMEM((2, height, TILE), jnp.float32),
            pltpu.VMEM((2, TILE, height), jnp.float32),
            pltpu.VMEM((2, height, TILE), jnp.float32),
            pltpu.VMEM((2, TILE, height), jnp.float32),
            pltpu.SemaphoreType.DMA,
        ] + [pltpu.SemaphoreType.DMA((2,))] * 5,
        compiler_params=pltpu.CompilerParams(vmem_limit_bytes=48 * 2**20),
        cost_estimate=pl.CostEstimate(
            flops=2 * n_slabs * width * height * (height + done), bytes_accessed=8 * area + 2 * n_slabs * width * (height + done),
            transcendentals=0),
        name="left_update",
    )(*operands)


def side_kernel(first, slabs_ref, own_ref, root_ref, left_root_ref, stat_ref, dir_in_ref, right_ref, dir_ref, precond):
    @pl.when(pl.program_id(0) == 0)
    def _():
        block = jnp.concatenate([slabs_ref[j] for j in range(slabs_ref.shape[0])], axis=1)
        precond[...] = lax.dot_general(block, root_ref[...], NT, preferred_element_type=jnp.float32).astype(precond.dtype)
        prod = lax.dot_general(own_ref[...], block, TN, preferred_element_type=jnp.float32)
        scale = EMA_DECAY if first else 1.0
        right_ref[...] = scale * stat_ref[...] + (1.0 - EMA_DECAY) * prod

    part = jnp.dot(left_root_ref[...], precond[...], preferred_element_type=jnp.float32)
    dir_ref[...] = part if first else dir_in_ref[...] + part


def side_update(index, sizes, group_slabs, own, root, left_root, stat, direction):
    height = sizes[index]
    rows, width = left_root.shape[0], own.shape[1]
    tile_m = rows // 8
    first = direction is None
    if first:
        direction = jnp.zeros((8, 128), jnp.float32)
        dir_spec = pl.BlockSpec((8, 128), lambda m: (0, 0))
    else:
        dir_spec = pl.BlockSpec((tile_m, width), lambda m: (m, 0))
    base = sum(sizes[:index])
    col_block = base // height
    return pl.pallas_call(
        functools.partial(side_kernel, first),
        grid=(rows // tile_m,),
        out_shape=(jax.ShapeDtypeStruct(stat.shape, jnp.float32), jax.ShapeDtypeStruct((rows, width), jnp.float32)),
        in_specs=[
            pl.BlockSpec(group_slabs.shape, lambda m: (0, 0, 0)),
            pl.BlockSpec((height, width), lambda m: (col_block, 0)),
            pl.BlockSpec(root.shape, lambda m: (0, 0)),
            pl.BlockSpec((tile_m, height), lambda m: (m, col_block)),
            pl.BlockSpec(stat.shape, lambda m: (0, 0)),
            dir_spec,
        ],
        out_specs=(pl.BlockSpec(stat.shape, lambda m: (0, 0)), pl.BlockSpec((tile_m, width), lambda m: (m, 0))),
        scratch_shapes=[pltpu.VMEM((height, width), own.dtype)],
        compiler_params=pltpu.CompilerParams(vmem_limit_bytes=32 * 2**20, dimension_semantics=("arbitrary",)),
        cost_estimate=pl.CostEstimate(flops=2 * rows * height * width, bytes_accessed=2 * rows * height, transcendentals=0),
        name="side_update",
    )(group_slabs, own, root, left_root, stat, direction)


def solution(mesh):
    stat_spec = P('layer', None)
    shard_spec = P('layer', 'tensor')
    row_spec = P(('layer', 'tensor'), None)

    def local_step(gradient, left_stat, right_stat, left_root, right_root):
        rows, width = gradient.shape
        group_size = right_stat.shape[1] // width
        group_start = lax.axis_index('tensor') // group_size * group_size
        unit = rows // sum(ROW_PARTS)
        sizes = tuple(part * unit for part in ROW_PARTS)
        chunks, base = [], 0
        for size in sizes:
            chunks.append(lax.all_gather(gradient[base:base + size], 'tensor', axis=0))
            base += size
        left_new, right_new, direction = None, right_stat, None
        for index in range(len(sizes)):
            left_new = left_update(index, sizes, chunks[:index + 1], left_stat, left_new)
            group_slabs = lax.dynamic_slice_in_dim(chunks[index], group_start, group_size, axis=0)
            right_new, direction = side_update(
                index, sizes, group_slabs, gradient, right_root, left_root, right_new, direction)
        return left_new, right_new, direction

    return jax.shard_map(local_step, mesh=mesh, in_specs=(shard_spec, stat_spec, row_spec, stat_spec, row_spec), out_specs=(stat_spec, row_spec, shard_spec), check_vma=False)
```

```python
import functools

import jax
import jax.numpy as jnp
from jax import lax
from jax.experimental import pallas as pl
from jax.experimental.pallas import tpu as pltpu
from jax.sharding import PartitionSpec as P

EMA_DECAY = 0.9
CORES = 2
HALF = 128
CHUNK = 2 * HALF
BATCH = 4
GROUP = 4
SLOTS = 4
NT = (((1,), (1,)), ((), ()))
TN = (((0,), (0,)), ((), ()))
HBM = pl.BlockSpec(memory_space=pltpu.HBM)


def gather_kernel(nx, ny, grad_ref, root_ref, stat_ref, left_root_ref, prod_ref, right_ref, dir_ref,
                  gath, acc, acc_rem, root, right_acc, dir_acc, left_root, precond,
                  p1_recv, p1_send, p2_recv, p2_send, plane_recv, plane_send, prod_recv, prod_send, prod_local,
                  rem_send, rem_local, lr_sem, misc_sem):
    n_chunks = grad_ref.shape[0]
    n_batches = n_chunks // BATCH
    me = lax.axis_index('tensor')
    core = lax.rem(me, CORES)
    x = lax.rem(me // CORES, nx)
    y = me // (CORES * nx)
    xs = [lax.rem(x + d, nx) for d in range(nx)]
    ys = [lax.rem(y + d, ny) for d in range(ny)]

    def device(row, col, c):
        return {'tensor': (row * nx + col) * CORES + c}

    partner = device(y, x, 1 - core)
    targets = [device(y, xs[1], core), device(y, xs[-1], core), device(ys[1], x, core), device(ys[-1], x, core)]

    def remote(src, target, send, recv, dst=None):
        return pltpu.make_async_remote_copy(
            src_ref=src, dst_ref=src if dst is None else dst, send_sem=send, recv_sem=recv,
            device_id=target, device_id_type=pl.DeviceIdType.MESH)

    def p1_region(direction, hop, batch, back):
        half = direction // 2
        up = direction % 2 == 0
        shift = -back if up else back
        row, col = (y, xs[shift % nx]) if half == 0 else (ys[shift % ny], x)
        if hop == 0:
            span = pl.ds(batch * BATCH, BATCH)
        else:
            span = pl.ds(batch * BATCH + (0 if up else BATCH // 2), BATCH // 2)
        return gath.at[core, row, col, span, half]

    def p1_copy(direction, hop, batch, back):
        return remote(p1_region(direction, hop, batch, back), targets[direction],
                      p1_send.at[direction, hop], p1_recv.at[direction, hop, batch])

    def p2_region(direction, hop, chunk, back):
        half = 1 - direction // 2
        up = direction % 2 == 0
        shift = -back if up else back
        if half == 0:
            span = pl.ds(0, nx) if hop == 0 else pl.ds(0 if up else nx // 2, nx // 2)
            return gath.at[core, ys[shift % ny], span, chunk, half]
        span = pl.ds(0, ny) if hop == 0 else pl.ds(0 if up else ny // 2, ny // 2)
        return gath.at[core, span, xs[shift % nx], chunk, half]

    def p2_copy(direction, hop, chunk, back):
        return remote(p2_region(direction, hop, chunk, back), targets[direction],
                      p2_send.at[direction, hop], p2_recv.at[direction, hop, chunk])

    def plane_copy(chunk, plane):
        return remote(gath.at[plane, :, :, chunk], partner, plane_send, plane_recv.at[chunk])

    def lr_copy(chunk):
        slot = lax.rem(chunk, 2)
        return pltpu.make_async_copy(
            left_root_ref.at[:, pl.ds(pl.multiple_of(chunk * CHUNK, CHUNK), CHUNK)], left_root.at[slot], lr_sem.at[slot])

    own_copy = pltpu.make_async_copy(grad_ref, gath.at[core, y, x], misc_sem.at[0])
    root_copy = pltpu.make_async_copy(root_ref, root, misc_sem.at[1])
    stat_copy = pltpu.make_async_copy(stat_ref, right_acc, misc_sem.at[2])
    own_copy.start()
    root_copy.start()
    stat_copy.start()
    lr_copy(0).start()

    barrier = pltpu.get_barrier_semaphore()
    for target in targets + [partner]:
        pl.semaphore_signal(barrier, inc=1, device_id=target, device_id_type=pl.DeviceIdType.MESH)
    pl.semaphore_wait(barrier, len(targets) + 1)

    own_copy.wait()
    for batch in range(n_batches):
        for direction in range(4):
            p1_copy(direction, 0, batch, 0).start()
    for batch in range(n_batches):
        for direction in range(4):
            p1_copy(direction, 0, batch, 1).wait_recv()
        for direction in range(4):
            p1_copy(direction, 1, batch, 1).start()

    root_copy.wait()
    stat_copy.wait()
    right_acc[...] = EMA_DECAY * right_acc[...]
    dir_acc[...] = jnp.zeros_like(dir_acc)

    slabs = [(c, row, col) for c in range(CORES) for row in range(ny) for col in range(nx)]

    def tile(chunk, start, count):
        lhs = jnp.concatenate(
            [gath[c, row, col, pl.ds(start, count), core].reshape(count * HALF, -1) for c, row, col in slabs], axis=1)
        rhs = jnp.concatenate([gath[c, row, col, chunk].reshape(CHUNK, -1) for c, row, col in slabs], axis=1)
        out = lax.dot_general(lhs, rhs, NT, preferred_element_type=jnp.float32)
        return out.reshape(count, HALF, CHUNK)

    def full_out(slot, chunk, start):
        dst = prod_ref.at[chunk, pl.ds(start, GROUP), core]
        return (pltpu.make_async_copy(acc.at[slot], dst, prod_local.at[slot]),
                remote(acc.at[slot], partner, prod_send.at[slot], prod_recv, dst))

    def rem_out(chunk, start, count):
        dst = prod_ref.at[chunk, pl.ds(start, count), core]
        src = acc_rem.at[pl.ds(0, count)]
        return (pltpu.make_async_copy(src, dst, rem_local), remote(src, partner, rem_send, prod_recv, dst))

    def await_out(copies):
        copies[0].wait()
        copies[1].wait_send()

    def side(chunk):
        block = jnp.concatenate(
            [gath[c, y, col, chunk].reshape(CHUNK, -1) for col in range(nx) for c in range(CORES)], axis=1)
        own = gath[core, y, x, chunk].reshape(CHUNK, -1)
        precond[...] = lax.dot_general(block, root[...], NT, preferred_element_type=jnp.float32).astype(precond.dtype)
        right_acc[...] += (1.0 - EMA_DECAY) * lax.dot_general(own, block, TN, preferred_element_type=jnp.float32)
        slot = lax.rem(chunk, 2)
        lr_copy(chunk).wait()

        @pl.when(chunk + 1 < n_chunks)
        def _():
            lr_copy(chunk + 1).start()
        band = dir_acc.shape[0] // 8

        def bands(m, _):
            rows = pl.ds(pl.multiple_of(m * band, band), band)
            dir_acc[rows, :] += jnp.dot(left_root[slot, rows, :], precond[...], preferred_element_type=jnp.float32)
            return 0
        lax.fori_loop(0, 8, bands, 0)

    def products(chunk, done):
        count = (chunk + 1) // GROUP

        def full(g, t):
            slot = lax.rem(t, 2)

            @pl.when(t >= 2)
            def _():
                await_out(full_out(slot, 0, 0))
            acc[slot] = tile(chunk, g * GROUP, GROUP)
            for copy in full_out(slot, chunk, g * GROUP):
                copy.start()
            return t + 1
        done = lax.fori_loop(0, count, full, done)
        rest = lax.rem(chunk + 1, GROUP)
        for size in range(1, GROUP):
            before = size - 1 if size > 1 else GROUP - 1

            @pl.when(rest == size)
            def _(size=size, before=before):
                @pl.when(chunk >= GROUP if size == 1 else chunk >= 0)
                def _():
                    await_out(rem_out(0, 0, before))
                acc_rem[pl.ds(0, size)] = tile(chunk, count * GROUP, size)
                for copy in rem_out(chunk, count * GROUP, size):
                    copy.start()
        return done

    lead = 3

    def step(s, done):
        k = s - lead
        ahead = k + lead

        @pl.when(ahead < n_chunks)
        def _():
            @pl.when(lax.rem(ahead, BATCH) == 0)
            def _():
                batch = ahead // BATCH
                for direction in range(4):
                    p1_copy(direction, 1, batch, 2).wait_recv()
            for direction in range(4):
                p2_copy(direction, 0, ahead, 0).start()

        @pl.when(jnp.logical_and(k + 1 >= 0, k + 1 < n_chunks))
        def _():
            for direction in range(4):
                p2_copy(direction, 0, k + 1, 1).wait_recv()
            for direction in range(4):
                p2_copy(direction, 1, k + 1, 1).start()

        @pl.when(jnp.logical_and(k >= 0, k < n_chunks))
        def _():
            for direction in range(4):
                p2_copy(direction, 1, k, 2).wait_recv()
            plane_copy(k, core).start()

        @pl.when(k >= 1)
        def _():
            plane_copy(k - 1, 1 - core).wait_recv()
            side(k - 1)
        return lax.cond(k >= 1, lambda d: products(k - 1, d), lambda d: d, done)

    lax.fori_loop(0, n_chunks + lead + 1, step, 0)

    right_out = pltpu.make_async_copy(right_acc, right_ref, misc_sem.at[0])
    dir_out = pltpu.make_async_copy(dir_acc, dir_ref, misc_sem.at[1])
    right_out.start()
    dir_out.start()
    for slot in range(2):
        await_out(full_out(slot, 0, 0))
    await_out(rem_out(0, 0, GROUP - 1))
    tiles = prod_ref.at[pl.ds(0, n_chunks // 2), :, 0]
    remote(tiles, partner, prod_send.at[0], prod_recv).wait_recv()
    for direction in range(4):
        half = direction // 2
        remote(gath.at[core, y, x, :, half], partner, p1_send.at[direction, 0], p1_recv.at[0, 0, 0]).wait_send()
        remote(gath.at[core, y, x, pl.ds(0, n_chunks // 2), half], partner, p1_send.at[direction, 1], p1_recv.at[0, 0, 0]).wait_send()
        remote(gath.at[core, y, :, :, 0], partner, p2_send.at[direction, 0], p1_recv.at[0, 0, 0]).wait_send()
        remote(gath.at[core, y, pl.ds(0, nx // 2), :, 0], partner, p2_send.at[direction, 1], p1_recv.at[0, 0, 0]).wait_send()
    remote(gath.at[core], partner, plane_send, p1_recv.at[0, 0, 0]).wait_send()
    right_out.wait()
    dir_out.wait()


def gather_products(mesh, gradient, right_root, right_stat, left_root):
    rows, width = gradient.shape
    n_chunks = rows // CHUNK
    n_devices = mesh.shape['tensor']
    group = right_stat.shape[1] // width
    nx, ny = group // CORES, n_devices // group
    dma = pltpu.SemaphoreType.DMA
    slabs = n_devices
    return pl.pallas_call(
        functools.partial(gather_kernel, nx, ny),
        out_shape=(
            jax.ShapeDtypeStruct((n_chunks, n_chunks + 1, 2, HALF, CHUNK), jnp.float32),
            jax.ShapeDtypeStruct(right_stat.shape, jnp.float32),
            jax.ShapeDtypeStruct((rows, width), jnp.float32),
        ),
        in_specs=[HBM] * 4,
        out_specs=(HBM,) * 3,
        scratch_shapes=[
            pltpu.VMEM((CORES, ny, nx, n_chunks, 2, HALF, width), gradient.dtype),
            pltpu.VMEM((2, GROUP, HALF, CHUNK), jnp.float32),
            pltpu.VMEM((GROUP - 1, HALF, CHUNK), jnp.float32),
            pltpu.VMEM(right_root.shape, right_root.dtype),
            pltpu.VMEM(right_stat.shape, jnp.float32),
            pltpu.VMEM((rows, width), jnp.float32),
            pltpu.VMEM((2, rows, CHUNK), left_root.dtype),
            pltpu.VMEM((CHUNK, width), gradient.dtype),
            dma((4, 2, n_chunks // BATCH)), dma((4, 2)), dma((4, 2, n_chunks)), dma((4, 2)),
            dma((n_chunks,)), dma, dma, dma((2,)), dma((2,)), dma, dma, dma((2,)), dma((3,)),
        ],
        compiler_params=pltpu.CompilerParams(collective_id=0, has_side_effects=True, vmem_limit_bytes=60 * 2**20),
        cost_estimate=pl.CostEstimate(
            flops=rows * rows * slabs * width, bytes_accessed=4 * rows * rows, transcendentals=0),
        name='gather_products',
    )(gradient.reshape(n_chunks, 2, HALF, width), right_root, right_stat, left_root)


def left_kernel(left_ref, prod_ref, out_ref, in_a, in_b, in_p, out_a, out_b, a_sem, b_sem, p_sem, oa_sem, ob_sem):
    unit = 2 * CHUNK
    n = left_ref.shape[0] // unit
    total = n * (n + 1) // 2

    def place(i):
        first = lax.rem(i, n)
        second = lax.rem(first + i // n, n)
        return jnp.minimum(first, second), jnp.maximum(first, second)

    def window(ref, row, col):
        return ref.at[pl.ds(pl.multiple_of(row * unit, unit), unit), pl.ds(pl.multiple_of(col * unit, unit), unit)]

    def a_in(i, slot):
        low, high = place(i)
        return pltpu.make_async_copy(window(left_ref, low, high), in_a.at[slot], a_sem.at[slot])

    def b_in(i, slot):
        low, high = place(i)
        return pltpu.make_async_copy(window(left_ref, high, low), in_b.at[slot], b_sem.at[slot])

    def p_in(i, slot):
        low, high = place(i)
        return pltpu.make_async_copy(prod_ref.at[pl.ds(high * 2, 2), pl.ds(low * 2, 2)], in_p.at[slot], p_sem.at[slot])

    def a_out(i, slot):
        low, high = place(i)
        return pltpu.make_async_copy(out_a.at[slot], window(out_ref, low, high), oa_sem.at[slot])

    def b_out(i, slot):
        low, high = place(i)
        return pltpu.make_async_copy(out_b.at[slot], window(out_ref, high, low), ob_sem.at[slot])

    def fetch(i):
        slot = lax.rem(i, SLOTS)
        a_in(i, slot).start()
        p_in(i, slot).start()

        @pl.when(i >= n)
        def _():
            b_in(i, slot).start()

    for i in range(SLOTS - 1):
        fetch(i)

    def step(i, _):
        slot = lax.rem(i, SLOTS)

        @pl.when(i + SLOTS - 1 < total)
        def _():
            fetch(i + SLOTS - 1)

        a_in(i, slot).wait()
        p_in(i, slot).wait()

        @pl.when(i >= n)
        def _():
            b_in(i, slot).wait()

        @pl.when(i >= SLOTS)
        def _():
            a_out(i, slot).wait()

        @pl.when(i >= n + SLOTS)
        def _():
            b_out(i, slot).wait()

        def part(k, s):
            return in_p[slot, k, s].reshape(CHUNK, CHUNK)

        def mix(stat, prod):
            return EMA_DECAY * stat + (1.0 - EMA_DECAY) * prod

        spans = [slice(0, CHUNK), slice(CHUNK, unit)]

        @pl.when(i < n)
        def _():
            for r in range(2):
                for c in range(2):
                    prod = part(c, r) if c >= r else part(r, c).T
                    out_a[slot, spans[r], spans[c]] = mix(in_a[slot, spans[r], spans[c]], prod)

        @pl.when(i >= n)
        def _():
            for r in range(2):
                for c in range(2):
                    out_a[slot, spans[r], spans[c]] = mix(in_a[slot, spans[r], spans[c]], part(c, r))
                    out_b[slot, spans[c], spans[r]] = mix(in_b[slot, spans[c], spans[r]], part(c, r).T)
            b_out(i, slot).start()
        a_out(i, slot).start()
        return 0

    lax.fori_loop(0, total, step, 0)
    for slot in range(SLOTS):
        a_out(0, slot).wait()
        b_out(0, slot).wait()


def left_update(left_stat, prod):
    rows = left_stat.shape[0]
    block = (SLOTS, 2 * CHUNK, 2 * CHUNK)
    dma = pltpu.SemaphoreType.DMA
    return pl.pallas_call(
        left_kernel,
        out_shape=jax.ShapeDtypeStruct(left_stat.shape, left_stat.dtype),
        in_specs=[HBM] * 2,
        out_specs=HBM,
        scratch_shapes=[
            pltpu.VMEM(block, jnp.float32), pltpu.VMEM(block, jnp.float32),
            pltpu.VMEM((SLOTS, 2, 2, 2, HALF, CHUNK), jnp.float32),
            pltpu.VMEM(block, jnp.float32), pltpu.VMEM(block, jnp.float32),
        ] + [dma((SLOTS,))] * 5,
        compiler_params=pltpu.CompilerParams(vmem_limit_bytes=48 * 2**20),
        cost_estimate=pl.CostEstimate(flops=4 * rows * rows, bytes_accessed=10 * rows * rows, transcendentals=0),
        name='left_update',
    )(left_stat, prod)


def solution(mesh):
    stat_spec = P('layer', None)
    shard_spec = P('layer', 'tensor')
    row_spec = P(('layer', 'tensor'), None)

    def local_step(gradient, left_stat, right_stat, left_root, right_root):
        prod, right_new, direction = gather_products(mesh, gradient, right_root, right_stat, left_root)
        left_new = left_update(left_stat, prod)
        return left_new, right_new, direction

    return jax.shard_map(local_step, mesh=mesh, in_specs=(shard_spec, stat_spec, row_spec, stat_spec, row_spec), out_specs=(stat_spec, row_spec, shard_spec), check_vma=False)
```

```python
import functools

import jax
import jax.numpy as jnp
from jax import lax
from jax.experimental import pallas as pl
from jax.experimental.pallas import tpu as pltpu
from jax.sharding import PartitionSpec as P

EMA_DECAY = 0.9
CORES = 2
HALF = 128
CHUNK = 2 * HALF
BATCH = 2
GROUP = 4
SLOTS = 4
NT = (((1,), (1,)), ((), ()))
TN = (((0,), (0,)), ((), ()))
HBM = pl.BlockSpec(memory_space=pltpu.HBM)


def gather_kernel(nx, ny, grad_ref, root_ref, stat_ref, left_root_ref, prod_ref, right_ref, dir_ref,
                  gath, acc, acc_rem, root, right_acc, dir_acc, left_root, precond,
                  p1_recv, p1_send, p2_recv, p2_send, plane_recv, plane_send, prod_recv, prod_send, prod_local,
                  rem_send, rem_local, lr_sem, misc_sem):
    n_chunks = grad_ref.shape[0]
    n_batches = n_chunks // BATCH
    me = lax.axis_index('tensor')
    core = lax.rem(me, CORES)
    x = lax.rem(me // CORES, nx)
    y = me // (CORES * nx)
    xs = [lax.rem(x + d, nx) for d in range(nx)]
    ys = [lax.rem(y + d, ny) for d in range(ny)]

    def device(row, col, c):
        return {'tensor': (row * nx + col) * CORES + c}

    partner = device(y, x, 1 - core)
    targets = [device(y, xs[1], core), device(y, xs[-1], core), device(ys[1], x, core), device(ys[-1], x, core)]

    def remote(src, target, send, recv, dst=None):
        return pltpu.make_async_remote_copy(
            src_ref=src, dst_ref=src if dst is None else dst, send_sem=send, recv_sem=recv,
            device_id=target, device_id_type=pl.DeviceIdType.MESH)

    def p1_region(direction, hop, batch, back):
        half = direction // 2
        up = direction % 2 == 0
        shift = -back if up else back
        row, col = (y, xs[shift % nx]) if half == 0 else (ys[shift % ny], x)
        if hop == 0:
            span = pl.ds(batch * BATCH, BATCH)
        else:
            span = pl.ds(batch * BATCH + (0 if up else BATCH // 2), BATCH // 2)
        return gath.at[core, row, col, span, half]

    def p1_copy(direction, hop, batch, back):
        return remote(p1_region(direction, hop, batch, back), targets[direction],
                      p1_send.at[direction, hop], p1_recv.at[direction, hop, batch])

    def p2_region(direction, hop, chunk, back):
        half = 1 - direction // 2
        up = direction % 2 == 0
        shift = -back if up else back
        if half == 0:
            span = pl.ds(0, nx) if hop == 0 else pl.ds(0 if up else nx // 2, nx // 2)
            return gath.at[core, ys[shift % ny], span, chunk, half]
        span = pl.ds(0, ny) if hop == 0 else pl.ds(0 if up else ny // 2, ny // 2)
        return gath.at[core, span, xs[shift % nx], chunk, half]

    def p2_copy(direction, hop, chunk, back):
        return remote(p2_region(direction, hop, chunk, back), targets[direction],
                      p2_send.at[direction, hop], p2_recv.at[direction, hop, chunk])

    def plane_copy(chunk, plane):
        return remote(gath.at[plane, :, :, chunk], partner, plane_send, plane_recv.at[chunk])

    def lr_copy(batch):
        slot = lax.rem(batch, 2)
        width = BATCH * CHUNK
        return pltpu.make_async_copy(
            left_root_ref.at[:, pl.ds(pl.multiple_of(batch * width, width), width)], left_root.at[slot], lr_sem.at[slot])

    own_copy = pltpu.make_async_copy(grad_ref, gath.at[core, y, x], misc_sem.at[0])
    root_copy = pltpu.make_async_copy(root_ref, root, misc_sem.at[1])
    stat_copy = pltpu.make_async_copy(stat_ref, right_acc, misc_sem.at[2])
    own_copy.start()
    root_copy.start()
    stat_copy.start()
    lr_copy(0).start()

    barrier = pltpu.get_barrier_semaphore()
    for target in targets + [partner]:
        pl.semaphore_signal(barrier, inc=1, device_id=target, device_id_type=pl.DeviceIdType.MESH)
    pl.semaphore_wait(barrier, len(targets) + 1)

    own_copy.wait()
    lead_in = min(3, n_batches)
    for batch in range(lead_in):
        for direction in range(4):
            p1_copy(direction, 0, batch, 0).start()

    def p1_forward(batch):
        for direction in range(4):
            p1_copy(direction, 0, batch, 1).wait_recv()
        for direction in range(4):
            p1_copy(direction, 1, batch, 1).start()

    for batch in range(lead_in - 1):
        p1_forward(batch)

    root_copy.wait()
    stat_copy.wait()
    right_acc[...] = EMA_DECAY * right_acc[...]
    dir_acc[...] = jnp.zeros_like(dir_acc)

    slabs = [(c, row, col) for c in range(CORES) for row in range(ny) for col in range(nx)]

    def tile(chunk, start, count):
        lhs = jnp.concatenate(
            [gath[c, row, col, pl.ds(start, count), core].reshape(count * HALF, -1) for c, row, col in slabs], axis=1)
        rhs = jnp.concatenate([gath[c, row, col, chunk].reshape(CHUNK, -1) for c, row, col in slabs], axis=1)
        out = lax.dot_general(lhs, rhs, NT, preferred_element_type=jnp.float32)
        return out.reshape(count, HALF, CHUNK)

    def full_out(slot, chunk, start):
        dst = prod_ref.at[chunk, pl.ds(start, GROUP), core]
        return (pltpu.make_async_copy(acc.at[slot], dst, prod_local.at[slot]),
                remote(acc.at[slot], partner, prod_send.at[slot], prod_recv, dst))

    def rem_out(chunk, start, count):
        dst = prod_ref.at[chunk, pl.ds(start, count), core]
        src = acc_rem.at[pl.ds(0, count)]
        return (pltpu.make_async_copy(src, dst, rem_local), remote(src, partner, rem_send, prod_recv, dst))

    def await_out(copies):
        copies[0].wait()
        copies[1].wait_send()

    def side(batch):
        span = pl.ds(batch * BATCH, BATCH)
        block = jnp.concatenate(
            [gath[c, y, col, span].reshape(BATCH * CHUNK, -1) for col in range(nx) for c in range(CORES)], axis=1)
        own = gath[core, y, x, span].reshape(BATCH * CHUNK, -1)
        precond[...] = lax.dot_general(block, root[...], NT, preferred_element_type=jnp.float32).astype(precond.dtype)
        right_acc[...] += (1.0 - EMA_DECAY) * lax.dot_general(own, block, TN, preferred_element_type=jnp.float32)
        slot = lax.rem(batch, 2)
        lr_copy(batch).wait()

        @pl.when(batch + 1 < n_batches)
        def _():
            lr_copy(batch + 1).start()
        band = dir_acc.shape[0] // 4
        for m in range(4):
            rows = slice(m * band, (m + 1) * band)
            dir_acc[rows, :] += jnp.dot(left_root[slot, rows, :], precond[...], preferred_element_type=jnp.float32)

    def products(chunk, done):
        count = (chunk + 1) // GROUP

        def full(g, t):
            slot = lax.rem(t, 2)

            @pl.when(t >= 2)
            def _():
                await_out(full_out(slot, 0, 0))
            acc[slot] = tile(chunk, g * GROUP, GROUP)
            for copy in full_out(slot, chunk, g * GROUP):
                copy.start()
            return t + 1
        done = lax.fori_loop(0, count, full, done)
        rest = lax.rem(chunk + 1, GROUP)
        for size in range(1, GROUP):
            before = size - 1 if size > 1 else GROUP - 1

            @pl.when(rest == size)
            def _(size=size, before=before):
                @pl.when(chunk >= GROUP if size == 1 else chunk >= 0)
                def _():
                    await_out(rem_out(0, 0, before))
                acc_rem[pl.ds(0, size)] = tile(chunk, count * GROUP, size)
                for copy in rem_out(chunk, count * GROUP, size):
                    copy.start()
        return done

    lead = 3

    def step(s, done):
        k = s - lead
        ahead = k + lead

        @pl.when(ahead < n_chunks)
        def _():
            batch = ahead // BATCH

            @pl.when(lax.rem(ahead, BATCH) == 0)
            def _():
                for direction in range(4):
                    p1_copy(direction, 1, batch, 2).wait_recv()
            for direction in range(4):
                p2_copy(direction, 0, ahead, 0).start()

            @pl.when(jnp.logical_and(lax.rem(ahead, BATCH) == 0, batch + lead_in < n_batches))
            def _():
                for direction in range(4):
                    p1_copy(direction, 0, batch + lead_in, 0).start()

            @pl.when(jnp.logical_and(lax.rem(ahead, BATCH) == 1, batch + lead_in - 1 < n_batches))
            def _():
                p1_forward(batch + lead_in - 1)

        @pl.when(jnp.logical_and(k + 1 >= 0, k + 1 < n_chunks))
        def _():
            for direction in range(4):
                p2_copy(direction, 0, k + 1, 1).wait_recv()
            for direction in range(4):
                p2_copy(direction, 1, k + 1, 1).start()

        @pl.when(jnp.logical_and(k >= 0, k < n_chunks))
        def _():
            for direction in range(4):
                p2_copy(direction, 1, k, 2).wait_recv()
            plane_copy(k, core).start()

        @pl.when(k >= 1)
        def _():
            plane_copy(k - 1, 1 - core).wait_recv()

            @pl.when(lax.rem(k, BATCH) == 0)
            def _():
                side(k // BATCH - 1)
        return lax.cond(k >= 1, lambda d: products(k - 1, d), lambda d: d, done)

    lax.fori_loop(0, n_chunks + lead + 1, step, 0)

    right_out = pltpu.make_async_copy(right_acc, right_ref, misc_sem.at[0])
    dir_out = pltpu.make_async_copy(dir_acc, dir_ref, misc_sem.at[1])
    right_out.start()
    dir_out.start()
    for slot in range(2):
        await_out(full_out(slot, 0, 0))
    await_out(rem_out(0, 0, GROUP - 1))
    tiles = prod_ref.at[pl.ds(0, n_chunks // 2), :, 0]
    remote(tiles, partner, prod_send.at[0], prod_recv).wait_recv()
    for direction in range(4):
        half = direction // 2
        remote(gath.at[core, y, x, :, half], partner, p1_send.at[direction, 0], p1_recv.at[0, 0, 0]).wait_send()
        remote(gath.at[core, y, x, pl.ds(0, n_chunks // 2), half], partner, p1_send.at[direction, 1], p1_recv.at[0, 0, 0]).wait_send()
        remote(gath.at[core, y, :, :, 0], partner, p2_send.at[direction, 0], p1_recv.at[0, 0, 0]).wait_send()
        remote(gath.at[core, y, pl.ds(0, nx // 2), :, 0], partner, p2_send.at[direction, 1], p1_recv.at[0, 0, 0]).wait_send()
    remote(gath.at[core], partner, plane_send, p1_recv.at[0, 0, 0]).wait_send()
    right_out.wait()
    dir_out.wait()


def gather_products(mesh, gradient, right_root, right_stat, left_root):
    rows, width = gradient.shape
    n_chunks = rows // CHUNK
    n_devices = mesh.shape['tensor']
    group = right_stat.shape[1] // width
    nx, ny = group // CORES, n_devices // group
    dma = pltpu.SemaphoreType.DMA
    slabs = n_devices
    return pl.pallas_call(
        functools.partial(gather_kernel, nx, ny),
        out_shape=(
            jax.ShapeDtypeStruct((n_chunks, n_chunks + 1, 2, HALF, CHUNK), jnp.float32),
            jax.ShapeDtypeStruct(right_stat.shape, jnp.float32),
            jax.ShapeDtypeStruct((rows, width), jnp.float32),
        ),
        in_specs=[HBM] * 4,
        out_specs=(HBM,) * 3,
        scratch_shapes=[
            pltpu.VMEM((CORES, ny, nx, n_chunks, 2, HALF, width), gradient.dtype),
            pltpu.VMEM((2, GROUP, HALF, CHUNK), jnp.float32),
            pltpu.VMEM((GROUP - 1, HALF, CHUNK), jnp.float32),
            pltpu.VMEM(right_root.shape, right_root.dtype),
            pltpu.VMEM(right_stat.shape, jnp.float32),
            pltpu.VMEM((rows, width), jnp.float32),
            pltpu.VMEM((2, rows, BATCH * CHUNK), left_root.dtype),
            pltpu.VMEM((BATCH * CHUNK, width), gradient.dtype),
            dma((4, 2, n_chunks // BATCH)), dma((4, 2)), dma((4, 2, n_chunks)), dma((4, 2)),
            dma((n_chunks,)), dma, dma, dma((2,)), dma((2,)), dma, dma, dma((2,)), dma((3,)),
        ],
        compiler_params=pltpu.CompilerParams(collective_id=0, has_side_effects=True, vmem_limit_bytes=60 * 2**20),
        cost_estimate=pl.CostEstimate(
            flops=rows * rows * slabs * width, bytes_accessed=4 * rows * rows, transcendentals=0),
        name='gather_products',
    )(gradient.reshape(n_chunks, 2, HALF, width), right_root, right_stat, left_root)


def left_kernel(left_ref, prod_ref, out_ref, in_a, in_b, in_p, out_a, out_b, a_sem, b_sem, p_sem, oa_sem, ob_sem):
    unit = 2 * CHUNK
    n = left_ref.shape[0] // unit
    total = n * (n + 1) // 2

    def place(i):
        first = lax.rem(i, n)
        second = lax.rem(first + i // n, n)
        return jnp.minimum(first, second), jnp.maximum(first, second)

    def window(ref, row, col):
        return ref.at[pl.ds(pl.multiple_of(row * unit, unit), unit), pl.ds(pl.multiple_of(col * unit, unit), unit)]

    def a_in(i, slot):
        low, high = place(i)
        return pltpu.make_async_copy(window(left_ref, low, high), in_a.at[slot], a_sem.at[slot])

    def b_in(i, slot):
        low, high = place(i)
        return pltpu.make_async_copy(window(left_ref, high, low), in_b.at[slot], b_sem.at[slot])

    def p_in(i, slot):
        low, high = place(i)
        return pltpu.make_async_copy(prod_ref.at[pl.ds(high * 2, 2), pl.ds(low * 2, 2)], in_p.at[slot], p_sem.at[slot])

    def a_out(i, slot):
        low, high = place(i)
        return pltpu.make_async_copy(out_a.at[slot], window(out_ref, low, high), oa_sem.at[slot])

    def b_out(i, slot):
        low, high = place(i)
        return pltpu.make_async_copy(out_b.at[slot], window(out_ref, high, low), ob_sem.at[slot])

    def fetch(i):
        slot = lax.rem(i, SLOTS)
        a_in(i, slot).start()
        p_in(i, slot).start()

        @pl.when(i >= n)
        def _():
            b_in(i, slot).start()

    for i in range(SLOTS - 1):
        fetch(i)

    def step(i, _):
        slot = lax.rem(i, SLOTS)

        @pl.when(i + SLOTS - 1 < total)
        def _():
            fetch(i + SLOTS - 1)

        a_in(i, slot).wait()
        p_in(i, slot).wait()

        @pl.when(i >= n)
        def _():
            b_in(i, slot).wait()

        @pl.when(i >= SLOTS)
        def _():
            a_out(i, slot).wait()

        @pl.when(i >= n + SLOTS)
        def _():
            b_out(i, slot).wait()

        def part(k, s):
            return in_p[slot, k, s].reshape(CHUNK, CHUNK)

        def mix(stat, prod):
            return EMA_DECAY * stat + (1.0 - EMA_DECAY) * prod

        spans = [slice(0, CHUNK), slice(CHUNK, unit)]

        @pl.when(i < n)
        def _():
            for r in range(2):
                for c in range(2):
                    prod = part(c, r) if c >= r else part(r, c).T
                    out_a[slot, spans[r], spans[c]] = mix(in_a[slot, spans[r], spans[c]], prod)

        @pl.when(i >= n)
        def _():
            for r in range(2):
                for c in range(2):
                    out_a[slot, spans[r], spans[c]] = mix(in_a[slot, spans[r], spans[c]], part(c, r))
                    out_b[slot, spans[c], spans[r]] = mix(in_b[slot, spans[c], spans[r]], part(c, r).T)
            b_out(i, slot).start()
        a_out(i, slot).start()
        return 0

    lax.fori_loop(0, total, step, 0)
    for slot in range(SLOTS):
        a_out(0, slot).wait()
        b_out(0, slot).wait()


def left_update(left_stat, prod):
    rows = left_stat.shape[0]
    block = (SLOTS, 2 * CHUNK, 2 * CHUNK)
    dma = pltpu.SemaphoreType.DMA
    return pl.pallas_call(
        left_kernel,
        out_shape=jax.ShapeDtypeStruct(left_stat.shape, left_stat.dtype),
        in_specs=[HBM] * 2,
        out_specs=HBM,
        scratch_shapes=[
            pltpu.VMEM(block, jnp.float32), pltpu.VMEM(block, jnp.float32),
            pltpu.VMEM((SLOTS, 2, 2, 2, HALF, CHUNK), jnp.float32),
            pltpu.VMEM(block, jnp.float32), pltpu.VMEM(block, jnp.float32),
        ] + [dma((SLOTS,))] * 5,
        compiler_params=pltpu.CompilerParams(vmem_limit_bytes=48 * 2**20),
        cost_estimate=pl.CostEstimate(flops=4 * rows * rows, bytes_accessed=10 * rows * rows, transcendentals=0),
        name='left_update',
    )(left_stat, prod)


def solution(mesh):
    stat_spec = P('layer', None)
    shard_spec = P('layer', 'tensor')
    row_spec = P(('layer', 'tensor'), None)

    def local_step(gradient, left_stat, right_stat, left_root, right_root):
        prod, right_new, direction = gather_products(mesh, gradient, right_root, right_stat, left_root)
        left_new = left_update(left_stat, prod)
        return left_new, right_new, direction

    return jax.shard_map(local_step, mesh=mesh, in_specs=(shard_spec, stat_spec, row_spec, stat_spec, row_spec), out_specs=(stat_spec, row_spec, shard_spec), check_vma=False)
```

```python
import functools

import jax
import jax.numpy as jnp
from jax import lax
from jax.experimental import pallas as pl
from jax.experimental.pallas import tpu as pltpu
from jax.sharding import PartitionSpec as P

EMA_DECAY = 0.9
CORES = 2
HALF = 128
CHUNK = 2 * HALF
BATCH = 2
GROUP = 4
SLOTS = 4
NT = (((1,), (1,)), ((), ()))
TN = (((0,), (0,)), ((), ()))
HBM = pl.BlockSpec(memory_space=pltpu.HBM)


def gather_kernel(nx, ny, grad_ref, root_ref, stat_ref, left_root_ref, prod_ref, right_ref, dir_ref,
                  gath, acc, acc_rem, root, right_acc, dir_acc, left_root, precond,
                  p1_recv, p1_send, p2_recv, p2_send, plane_recv, plane_send, prod_recv, prod_send, prod_local,
                  rem_send, rem_local, lr_sem, misc_sem):
    n_chunks = grad_ref.shape[0]
    n_batches = n_chunks // BATCH
    me = lax.axis_index('tensor')
    core = lax.rem(me, CORES)
    x = lax.rem(me // CORES, nx)
    y = me // (CORES * nx)
    xs = [lax.rem(x + d, nx) for d in range(nx)]
    ys = [lax.rem(y + d, ny) for d in range(ny)]

    def device(row, col, c):
        return {'tensor': (row * nx + col) * CORES + c}

    partner = device(y, x, 1 - core)
    targets = [device(y, xs[1], core), device(y, xs[-1], core), device(ys[1], x, core), device(ys[-1], x, core)]

    def remote(src, target, send, recv, dst=None):
        return pltpu.make_async_remote_copy(
            src_ref=src, dst_ref=src if dst is None else dst, send_sem=send, recv_sem=recv,
            device_id=target, device_id_type=pl.DeviceIdType.MESH)

    def p1_region(direction, hop, batch, back):
        half = direction // 2
        up = direction % 2 == 0
        shift = -back if up else back
        row, col = (y, xs[shift % nx]) if half == 0 else (ys[shift % ny], x)
        if hop == 0:
            span = pl.ds(batch * BATCH, BATCH)
        else:
            span = pl.ds(batch * BATCH + (0 if up else BATCH // 2), BATCH // 2)
        return gath.at[core, row, col, span, half]

    def p1_copy(direction, hop, batch, back):
        return remote(p1_region(direction, hop, batch, back), targets[direction],
                      p1_send.at[direction, hop], p1_recv.at[direction, hop, batch])

    def p2_region(direction, hop, chunk, back):
        half = 1 - direction // 2
        up = direction % 2 == 0
        shift = -back if up else back
        if half == 0:
            span = pl.ds(0, nx) if hop == 0 else pl.ds(0 if up else nx // 2, nx // 2)
            return gath.at[core, ys[shift % ny], span, chunk, half]
        span = pl.ds(0, ny) if hop == 0 else pl.ds(0 if up else ny // 2, ny // 2)
        return gath.at[core, span, xs[shift % nx], chunk, half]

    def p2_copy(direction, hop, chunk, back):
        return remote(p2_region(direction, hop, chunk, back), targets[direction],
                      p2_send.at[direction, hop], p2_recv.at[direction, hop, chunk])

    def plane_copy(chunk, plane):
        return remote(gath.at[plane, :, :, chunk], partner, plane_send, plane_recv.at[chunk])

    def lr_copy(batch):
        slot = lax.rem(batch, 2)
        width = BATCH * CHUNK
        return pltpu.make_async_copy(
            left_root_ref.at[:, pl.ds(pl.multiple_of(batch * width, width), width)], left_root.at[slot], lr_sem.at[slot])

    own_copy = pltpu.make_async_copy(grad_ref, gath.at[core, y, x], misc_sem.at[0])
    root_copy = pltpu.make_async_copy(root_ref, root, misc_sem.at[1])
    stat_copy = pltpu.make_async_copy(stat_ref, right_acc, misc_sem.at[2])
    own_copy.start()
    root_copy.start()
    stat_copy.start()
    lr_copy(0).start()

    barrier = pltpu.get_barrier_semaphore()
    for target in targets + [partner]:
        pl.semaphore_signal(barrier, inc=1, device_id=target, device_id_type=pl.DeviceIdType.MESH)
    pl.semaphore_wait(barrier, len(targets) + 1)

    own_copy.wait()
    lead_in = min(3, n_batches)
    for batch in range(lead_in):
        for direction in range(4):
            p1_copy(direction, 0, batch, 0).start()

    def p1_forward(batch):
        for direction in range(4):
            p1_copy(direction, 0, batch, 1).wait_recv()
        for direction in range(4):
            p1_copy(direction, 1, batch, 1).start()

    for batch in range(lead_in - 1):
        p1_forward(batch)

    root_copy.wait()
    stat_copy.wait()
    right_acc[...] = EMA_DECAY * right_acc[...]
    dir_acc[...] = jnp.zeros_like(dir_acc)

    slabs = [(c, row, col) for c in range(CORES) for row in range(ny) for col in range(nx)]

    def tile(chunk, start, count):
        lhs = jnp.concatenate(
            [gath[c, row, col, pl.ds(start, count), core].reshape(count * HALF, -1) for c, row, col in slabs], axis=1)
        rhs = jnp.concatenate([gath[c, row, col, chunk].reshape(CHUNK, -1) for c, row, col in slabs], axis=1)
        out = lax.dot_general(lhs, rhs, NT, preferred_element_type=jnp.float32)
        return out.reshape(count, HALF, CHUNK)

    def full_out(slot, chunk, start):
        dst = prod_ref.at[chunk, pl.ds(start, GROUP), core]
        return (pltpu.make_async_copy(acc.at[slot], dst, prod_local.at[slot]),
                remote(acc.at[slot], partner, prod_send.at[slot], prod_recv, dst))

    def rem_out(chunk, start, count):
        dst = prod_ref.at[chunk, pl.ds(start, count), core]
        src = acc_rem.at[pl.ds(0, count)]
        return (pltpu.make_async_copy(src, dst, rem_local), remote(src, partner, rem_send, prod_recv, dst))

    def await_out(copies):
        copies[0].wait()
        copies[1].wait_send()

    def side(batch):
        span = pl.ds(batch * BATCH, BATCH)
        block = jnp.concatenate(
            [gath[c, y, col, span].reshape(BATCH * CHUNK, -1) for col in range(nx) for c in range(CORES)], axis=1)
        own = gath[core, y, x, span].reshape(BATCH * CHUNK, -1)
        precond[...] = lax.dot_general(block, root[...], NT, preferred_element_type=jnp.float32).astype(precond.dtype)
        right_acc[...] += (1.0 - EMA_DECAY) * lax.dot_general(own, block, TN, preferred_element_type=jnp.float32)
        slot = lax.rem(batch, 2)
        lr_copy(batch).wait()

        @pl.when(batch + 1 < n_batches)
        def _():
            lr_copy(batch + 1).start()
        band = dir_acc.shape[0] // 4
        for m in range(4):
            rows = slice(m * band, (m + 1) * band)
            dir_acc[rows, :] += jnp.dot(left_root[slot, rows, :], precond[...], preferred_element_type=jnp.float32)

    def full(chunk, g, t):
        slot = lax.rem(t, 2)

        @pl.when(t >= 2)
        def _():
            await_out(full_out(slot, 0, 0))
        acc[slot] = tile(chunk, g * GROUP, GROUP)
        for copy in full_out(slot, chunk, g * GROUP):
            copy.start()
        return t + 1

    def rest(chunk):
        count = (chunk + 1) // GROUP
        left = lax.rem(chunk + 1, GROUP)
        for size in range(1, GROUP):
            before = size - 1 if size > 1 else GROUP - 1

            @pl.when(left == size)
            def _(size=size, before=before):
                @pl.when(chunk >= GROUP if size == 1 else chunk >= 0)
                def _():
                    await_out(rem_out(0, 0, before))
                acc_rem[pl.ds(0, size)] = tile(chunk, count * GROUP, size)
                for copy in rem_out(chunk, count * GROUP, size):
                    copy.start()

    lead = 3

    def step(s, done):
        k = s - lead
        ahead = k + lead

        @pl.when(ahead < n_chunks)
        def _():
            batch = ahead // BATCH

            @pl.when(lax.rem(ahead, BATCH) == 0)
            def _():
                for direction in range(4):
                    p1_copy(direction, 1, batch, 2).wait_recv()
            for direction in range(4):
                p2_copy(direction, 0, ahead, 0).start()

            @pl.when(jnp.logical_and(lax.rem(ahead, BATCH) == 0, batch + lead_in < n_batches))
            def _():
                for direction in range(4):
                    p1_copy(direction, 0, batch + lead_in, 0).start()

            @pl.when(jnp.logical_and(lax.rem(ahead, BATCH) == 1, batch + lead_in - 1 < n_batches))
            def _():
                p1_forward(batch + lead_in - 1)

        @pl.when(jnp.logical_and(k >= 0, k < n_chunks))
        def _():
            for direction in range(4):
                p2_copy(direction, 1, k, 2).wait_recv()
            plane_copy(k, core).start()

        @pl.when(k >= 1)
        def _():
            plane_copy(k - 1, 1 - core).wait_recv()

            @pl.when(lax.rem(k, BATCH) == 0)
            def _():
                side(k // BATCH - 1)
            rest(k - 1)
        count = jnp.maximum(k, 0) // GROUP
        done = lax.fori_loop(0, count // 2, functools.partial(full, k - 1), done)

        @pl.when(jnp.logical_and(k + 2 >= 0, k + 2 < n_chunks))
        def _():
            for direction in range(4):
                p2_copy(direction, 0, k + 2, 1).wait_recv()
            for direction in range(4):
                p2_copy(direction, 1, k + 2, 1).start()
        return lax.fori_loop(count // 2, count, functools.partial(full, k - 1), done)

    lax.fori_loop(0, n_chunks + lead + 1, step, 0)

    right_out = pltpu.make_async_copy(right_acc, right_ref, misc_sem.at[0])
    dir_out = pltpu.make_async_copy(dir_acc, dir_ref, misc_sem.at[1])
    right_out.start()
    dir_out.start()
    for slot in range(2):
        await_out(full_out(slot, 0, 0))
    await_out(rem_out(0, 0, GROUP - 1))
    tiles = prod_ref.at[pl.ds(0, n_chunks // 2), :, 0]
    remote(tiles, partner, prod_send.at[0], prod_recv).wait_recv()
    for direction in range(4):
        half = direction // 2
        remote(gath.at[core, y, x, :, half], partner, p1_send.at[direction, 0], p1_recv.at[0, 0, 0]).wait_send()
        remote(gath.at[core, y, x, pl.ds(0, n_chunks // 2), half], partner, p1_send.at[direction, 1], p1_recv.at[0, 0, 0]).wait_send()
        remote(gath.at[core, y, :, :, 0], partner, p2_send.at[direction, 0], p1_recv.at[0, 0, 0]).wait_send()
        remote(gath.at[core, y, pl.ds(0, nx // 2), :, 0], partner, p2_send.at[direction, 1], p1_recv.at[0, 0, 0]).wait_send()
    remote(gath.at[core], partner, plane_send, p1_recv.at[0, 0, 0]).wait_send()
    right_out.wait()
    dir_out.wait()


def gather_products(mesh, gradient, right_root, right_stat, left_root):
    rows, width = gradient.shape
    n_chunks = rows // CHUNK
    n_devices = mesh.shape['tensor']
    group = right_stat.shape[1] // width
    nx, ny = group // CORES, n_devices // group
    dma = pltpu.SemaphoreType.DMA
    slabs = n_devices
    return pl.pallas_call(
        functools.partial(gather_kernel, nx, ny),
        out_shape=(
            jax.ShapeDtypeStruct((n_chunks, n_chunks + 1, 2, HALF, CHUNK), jnp.float32),
            jax.ShapeDtypeStruct(right_stat.shape, jnp.float32),
            jax.ShapeDtypeStruct((rows, width), jnp.float32),
        ),
        in_specs=[HBM] * 4,
        out_specs=(HBM,) * 3,
        scratch_shapes=[
            pltpu.VMEM((CORES, ny, nx, n_chunks, 2, HALF, width), gradient.dtype),
            pltpu.VMEM((2, GROUP, HALF, CHUNK), jnp.float32),
            pltpu.VMEM((GROUP - 1, HALF, CHUNK), jnp.float32),
            pltpu.VMEM(right_root.shape, right_root.dtype),
            pltpu.VMEM(right_stat.shape, jnp.float32),
            pltpu.VMEM((rows, width), jnp.float32),
            pltpu.VMEM((2, rows, BATCH * CHUNK), left_root.dtype),
            pltpu.VMEM((BATCH * CHUNK, width), gradient.dtype),
            dma((4, 2, n_chunks // BATCH)), dma((4, 2)), dma((4, 2, n_chunks)), dma((4, 2)),
            dma((n_chunks,)), dma, dma, dma((2,)), dma((2,)), dma, dma, dma((2,)), dma((3,)),
        ],
        compiler_params=pltpu.CompilerParams(collective_id=0, has_side_effects=True, vmem_limit_bytes=60 * 2**20),
        cost_estimate=pl.CostEstimate(
            flops=rows * rows * slabs * width, bytes_accessed=4 * rows * rows, transcendentals=0),
        name='gather_products',
    )(gradient.reshape(n_chunks, 2, HALF, width), right_root, right_stat, left_root)


def left_kernel(left_ref, prod_ref, out_ref, in_a, in_b, in_p, out_a, out_b, a_sem, b_sem, p_sem, oa_sem, ob_sem):
    unit = 2 * CHUNK
    n = left_ref.shape[0] // unit
    total = n * (n + 1) // 2

    def place(i):
        first = lax.rem(i, n)
        second = lax.rem(first + i // n, n)
        return jnp.minimum(first, second), jnp.maximum(first, second)

    def window(ref, row, col):
        return ref.at[pl.ds(pl.multiple_of(row * unit, unit), unit), pl.ds(pl.multiple_of(col * unit, unit), unit)]

    def a_in(i, slot):
        low, high = place(i)
        return pltpu.make_async_copy(window(left_ref, low, high), in_a.at[slot], a_sem.at[slot])

    def b_in(i, slot):
        low, high = place(i)
        return pltpu.make_async_copy(window(left_ref, high, low), in_b.at[slot], b_sem.at[slot])

    def p_in(i, slot):
        low, high = place(i)
        return pltpu.make_async_copy(prod_ref.at[pl.ds(high * 2, 2), pl.ds(low * 2, 2)], in_p.at[slot], p_sem.at[slot])

    def a_out(i, slot):
        low, high = place(i)
        return pltpu.make_async_copy(out_a.at[slot], window(out_ref, low, high), oa_sem.at[slot])

    def b_out(i, slot):
        low, high = place(i)
        return pltpu.make_async_copy(out_b.at[slot], window(out_ref, high, low), ob_sem.at[slot])

    def fetch(i):
        slot = lax.rem(i, SLOTS)
        a_in(i, slot).start()
        p_in(i, slot).start()

        @pl.when(i >= n)
        def _():
            b_in(i, slot).start()

    for i in range(SLOTS - 1):
        fetch(i)

    def step(i, _):
        slot = lax.rem(i, SLOTS)

        @pl.when(i + SLOTS - 1 < total)
        def _():
            fetch(i + SLOTS - 1)

        a_in(i, slot).wait()
        p_in(i, slot).wait()

        @pl.when(i >= n)
        def _():
            b_in(i, slot).wait()

        @pl.when(i >= SLOTS)
        def _():
            a_out(i, slot).wait()

        @pl.when(i >= n + SLOTS)
        def _():
            b_out(i, slot).wait()

        def part(k, s):
            return in_p[slot, k, s].reshape(CHUNK, CHUNK)

        def mix(stat, prod):
            return EMA_DECAY * stat + (1.0 - EMA_DECAY) * prod

        spans = [slice(0, CHUNK), slice(CHUNK, unit)]

        @pl.when(i < n)
        def _():
            for r in range(2):
                for c in range(2):
                    prod = part(c, r) if c >= r else part(r, c).T
                    out_a[slot, spans[r], spans[c]] = mix(in_a[slot, spans[r], spans[c]], prod)

        @pl.when(i >= n)
        def _():
            for r in range(2):
                for c in range(2):
                    out_a[slot, spans[r], spans[c]] = mix(in_a[slot, spans[r], spans[c]], part(c, r))
                    out_b[slot, spans[c], spans[r]] = mix(in_b[slot, spans[c], spans[r]], part(c, r).T)
            b_out(i, slot).start()
        a_out(i, slot).start()
        return 0

    lax.fori_loop(0, total, step, 0)
    for slot in range(SLOTS):
        a_out(0, slot).wait()
        b_out(0, slot).wait()


def left_update(left_stat, prod):
    rows = left_stat.shape[0]
    block = (SLOTS, 2 * CHUNK, 2 * CHUNK)
    dma = pltpu.SemaphoreType.DMA
    return pl.pallas_call(
        left_kernel,
        out_shape=jax.ShapeDtypeStruct(left_stat.shape, left_stat.dtype),
        in_specs=[HBM] * 2,
        out_specs=HBM,
        scratch_shapes=[
            pltpu.VMEM(block, jnp.float32), pltpu.VMEM(block, jnp.float32),
            pltpu.VMEM((SLOTS, 2, 2, 2, HALF, CHUNK), jnp.float32),
            pltpu.VMEM(block, jnp.float32), pltpu.VMEM(block, jnp.float32),
        ] + [dma((SLOTS,))] * 5,
        compiler_params=pltpu.CompilerParams(vmem_limit_bytes=48 * 2**20),
        cost_estimate=pl.CostEstimate(flops=4 * rows * rows, bytes_accessed=10 * rows * rows, transcendentals=0),
        name='left_update',
    )(left_stat, prod)


def solution(mesh):
    stat_spec = P('layer', None)
    shard_spec = P('layer', 'tensor')
    row_spec = P(('layer', 'tensor'), None)

    def local_step(gradient, left_stat, right_stat, left_root, right_root):
        prod, right_new, direction = gather_products(mesh, gradient, right_root, right_stat, left_root)
        left_new = left_update(left_stat, prod)
        return left_new, right_new, direction

    return jax.shard_map(local_step, mesh=mesh, in_specs=(shard_spec, stat_spec, row_spec, stat_spec, row_spec), out_specs=(stat_spec, row_spec, shard_spec), check_vma=False)
```

```python
import functools

import jax
import jax.numpy as jnp
from jax import lax
from jax.experimental import pallas as pl
from jax.experimental.pallas import tpu as pltpu
from jax.sharding import PartitionSpec as P

EMA_DECAY = 0.9
CORES = 2
HALF = 128
CHUNK = 2 * HALF
BATCH = 2
GROUP = 4
SLOTS = 4
SCOPE = 57 * 2**19
NT = (((1,), (1,)), ((), ()))
TN = (((0,), (0,)), ((), ()))
HBM = pl.BlockSpec(memory_space=pltpu.HBM)
VMEM = pl.BlockSpec(memory_space=pltpu.VMEM)


def gather_kernel(nx, ny, grad_ref, root_ref, stat_ref, left_root_ref, prod_ref, gath, right_acc, dir_acc,
                  acc, acc_rem, root, left_root, precond,
                  p1_recv, p1_send, p2_recv, p2_send, plane_recv, plane_send, prod_recv, prod_send, prod_local,
                  rem_send, rem_local, lr_sem, misc_sem):
    n_chunks = grad_ref.shape[0]
    n_kept = prod_ref.shape[0]
    n_batches = n_chunks // BATCH
    me = lax.axis_index('tensor')
    core = lax.rem(me, CORES)
    x = lax.rem(me // CORES, nx)
    y = me // (CORES * nx)
    xs = [lax.rem(x + d, nx) for d in range(nx)]
    ys = [lax.rem(y + d, ny) for d in range(ny)]

    def device(row, col, c):
        return {'tensor': (row * nx + col) * CORES + c}

    partner = device(y, x, 1 - core)
    targets = [device(y, xs[1], core), device(y, xs[-1], core), device(ys[1], x, core), device(ys[-1], x, core)]

    def remote(src, target, send, recv, dst=None):
        return pltpu.make_async_remote_copy(
            src_ref=src, dst_ref=src if dst is None else dst, send_sem=send, recv_sem=recv,
            device_id=target, device_id_type=pl.DeviceIdType.MESH)

    def p1_region(direction, hop, batch, back):
        half = direction // 2
        up = direction % 2 == 0
        shift = -back if up else back
        row, col = (y, xs[shift % nx]) if half == 0 else (ys[shift % ny], x)
        if hop == 0:
            span = pl.ds(batch * BATCH, BATCH)
        else:
            span = pl.ds(batch * BATCH + (0 if up else BATCH // 2), BATCH // 2)
        return gath.at[core, row, col, span, half]

    def p1_copy(direction, hop, batch, back):
        return remote(p1_region(direction, hop, batch, back), targets[direction],
                      p1_send.at[direction, hop], p1_recv.at[direction, hop, batch])

    def p2_region(direction, hop, chunk, back):
        half = 1 - direction // 2
        up = direction % 2 == 0
        shift = -back if up else back
        if half == 0:
            span = pl.ds(0, nx) if hop == 0 else pl.ds(0 if up else nx // 2, nx // 2)
            return gath.at[core, ys[shift % ny], span, chunk, half]
        span = pl.ds(0, ny) if hop == 0 else pl.ds(0 if up else ny // 2, ny // 2)
        return gath.at[core, span, xs[shift % nx], chunk, half]

    def p2_copy(direction, hop, chunk, back):
        return remote(p2_region(direction, hop, chunk, back), targets[direction],
                      p2_send.at[direction, hop], p2_recv.at[direction, hop, chunk])

    def plane_copy(chunk, plane):
        return remote(gath.at[plane, :, :, chunk], partner, plane_send, plane_recv.at[chunk])

    def lr_copy(batch):
        slot = lax.rem(batch, 2)
        width = BATCH * CHUNK
        return pltpu.make_async_copy(
            left_root_ref.at[:, pl.ds(pl.multiple_of(batch * width, width), width)], left_root.at[slot], lr_sem.at[slot])

    own_copy = pltpu.make_async_copy(grad_ref, gath.at[core, y, x], misc_sem.at[0])
    root_copy = pltpu.make_async_copy(root_ref, root, misc_sem.at[1])
    stat_copy = pltpu.make_async_copy(stat_ref, right_acc, misc_sem.at[2])
    own_copy.start()
    root_copy.start()
    stat_copy.start()
    lr_copy(0).start()

    barrier = pltpu.get_barrier_semaphore()
    for target in targets + [partner]:
        pl.semaphore_signal(barrier, inc=1, device_id=target, device_id_type=pl.DeviceIdType.MESH)
    pl.semaphore_wait(barrier, len(targets) + 1)

    own_copy.wait()
    lead_in = min(3, n_batches)
    for batch in range(lead_in):
        for direction in range(4):
            p1_copy(direction, 0, batch, 0).start()

    def p1_forward(batch):
        for direction in range(4):
            p1_copy(direction, 0, batch, 1).wait_recv()
        for direction in range(4):
            p1_copy(direction, 1, batch, 1).start()

    for batch in range(lead_in - 1):
        p1_forward(batch)

    root_copy.wait()
    stat_copy.wait()
    right_acc[...] = EMA_DECAY * right_acc[...]
    dir_acc[...] = jnp.zeros_like(dir_acc)

    slabs = [(c, row, col) for c in range(CORES) for row in range(ny) for col in range(nx)]

    def tile(chunk, start, count):
        lhs = jnp.concatenate(
            [gath[c, row, col, pl.ds(start, count), core].reshape(count * HALF, -1) for c, row, col in slabs], axis=1)
        rhs = jnp.concatenate([gath[c, row, col, chunk].reshape(CHUNK, -1) for c, row, col in slabs], axis=1)
        out = lax.dot_general(lhs, rhs, NT, preferred_element_type=jnp.float32)
        return out.reshape(count, HALF, CHUNK)

    def full_out(slot, chunk, start):
        dst = prod_ref.at[chunk, pl.ds(start, GROUP), core]
        return (pltpu.make_async_copy(acc.at[slot], dst, prod_local.at[slot]),
                remote(acc.at[slot], partner, prod_send.at[slot], prod_recv, dst))

    def rem_out(chunk, start, count):
        dst = prod_ref.at[chunk, pl.ds(start, count), core]
        src = acc_rem.at[pl.ds(0, count)]
        return (pltpu.make_async_copy(src, dst, rem_local), remote(src, partner, rem_send, prod_recv, dst))

    def await_out(copies):
        copies[0].wait()
        copies[1].wait_send()

    def side(batch):
        span = pl.ds(batch * BATCH, BATCH)
        block = jnp.concatenate(
            [gath[c, y, col, span].reshape(BATCH * CHUNK, -1) for col in range(nx) for c in range(CORES)], axis=1)
        own = gath[core, y, x, span].reshape(BATCH * CHUNK, -1)
        precond[...] = lax.dot_general(block, root[...], NT, preferred_element_type=jnp.float32).astype(precond.dtype)
        right_acc[...] += (1.0 - EMA_DECAY) * lax.dot_general(own, block, TN, preferred_element_type=jnp.float32)
        slot = lax.rem(batch, 2)
        lr_copy(batch).wait()

        @pl.when(batch + 1 < n_batches)
        def _():
            lr_copy(batch + 1).start()
        band = dir_acc.shape[0] // 4
        for m in range(4):
            rows = slice(m * band, (m + 1) * band)
            dir_acc[rows, :] += jnp.dot(left_root[slot, rows, :], precond[...], preferred_element_type=jnp.float32)

    def full(chunk, g, t):
        slot = lax.rem(t, 2)

        @pl.when(t >= 2)
        def _():
            await_out(full_out(slot, 0, 0))
        acc[slot] = tile(chunk, g * GROUP, GROUP)
        for copy in full_out(slot, chunk, g * GROUP):
            copy.start()
        return t + 1

    def rest(chunk):
        count = (chunk + 1) // GROUP
        left = lax.rem(chunk + 1, GROUP)
        for size in range(1, GROUP):
            before = size - 1 if size > 1 else GROUP - 1

            @pl.when(left == size)
            def _(size=size, before=before):
                @pl.when(chunk >= GROUP if size == 1 else chunk >= 0)
                def _():
                    await_out(rem_out(0, 0, before))
                acc_rem[pl.ds(0, size)] = tile(chunk, count * GROUP, size)
                for copy in rem_out(chunk, count * GROUP, size):
                    copy.start()

    lead = 3

    def step(s, done):
        k = s - lead
        ahead = k + lead

        @pl.when(ahead < n_chunks)
        def _():
            batch = ahead // BATCH

            @pl.when(lax.rem(ahead, BATCH) == 0)
            def _():
                for direction in range(4):
                    p1_copy(direction, 1, batch, 2).wait_recv()
            for direction in range(4):
                p2_copy(direction, 0, ahead, 0).start()

            @pl.when(jnp.logical_and(lax.rem(ahead, BATCH) == 0, batch + lead_in < n_batches))
            def _():
                for direction in range(4):
                    p1_copy(direction, 0, batch + lead_in, 0).start()

            @pl.when(jnp.logical_and(lax.rem(ahead, BATCH) == 1, batch + lead_in - 1 < n_batches))
            def _():
                p1_forward(batch + lead_in - 1)

        @pl.when(jnp.logical_and(k >= 0, k < n_chunks))
        def _():
            for direction in range(4):
                p2_copy(direction, 1, k, 2).wait_recv()
            plane_copy(k, core).start()

        @pl.when(k >= 1)
        def _():
            plane_copy(k - 1, 1 - core).wait_recv()

            @pl.when(lax.rem(k, BATCH) == 0)
            def _():
                side(k // BATCH - 1)

            @pl.when(k - 1 < n_kept)
            def _():
                rest(k - 1)
        count = jnp.where(k - 1 < n_kept, jnp.maximum(k, 0) // GROUP, 0)
        done = lax.fori_loop(0, count // 2, functools.partial(full, k - 1), done)

        @pl.when(jnp.logical_and(k + 2 >= 0, k + 2 < n_chunks))
        def _():
            for direction in range(4):
                p2_copy(direction, 0, k + 2, 1).wait_recv()
            for direction in range(4):
                p2_copy(direction, 1, k + 2, 1).start()
        return lax.fori_loop(count // 2, count, functools.partial(full, k - 1), done)

    lax.fori_loop(0, n_chunks + lead + 1, step, 0)

    for slot in range(2):
        await_out(full_out(slot, 0, 0))
    await_out(rem_out(0, 0, n_kept % GROUP))
    tiles = prod_ref.at[pl.ds(0, n_kept // 2), :, 0]
    remote(tiles, partner, prod_send.at[0], prod_recv).wait_recv()
    for direction in range(4):
        half = direction // 2
        remote(gath.at[core, y, x, :, half], partner, p1_send.at[direction, 0], p1_recv.at[0, 0, 0]).wait_send()
        remote(gath.at[core, y, x, pl.ds(0, n_chunks // 2), half], partner, p1_send.at[direction, 1], p1_recv.at[0, 0, 0]).wait_send()
        remote(gath.at[core, y, :, :, 0], partner, p2_send.at[direction, 0], p1_recv.at[0, 0, 0]).wait_send()
        remote(gath.at[core, y, pl.ds(0, nx // 2), :, 0], partner, p2_send.at[direction, 1], p1_recv.at[0, 0, 0]).wait_send()
    remote(gath.at[core], partner, plane_send, p1_recv.at[0, 0, 0]).wait_send()


def gather_products(mesh, gradient, right_root, right_stat, left_root):
    rows, width = gradient.shape
    n_chunks = rows // CHUNK
    n_devices = mesh.shape['tensor']
    group = right_stat.shape[1] // width
    nx, ny = group // CORES, n_devices // group
    dma = pltpu.SemaphoreType.DMA
    slabs = n_devices
    operands = [pltpu.with_memory_space_constraint(a, pltpu.HBM) for a in (
        gradient.reshape(n_chunks, 2, HALF, width), right_root, right_stat, left_root)]
    return pl.pallas_call(
        functools.partial(gather_kernel, nx, ny),
        out_shape=(
            jax.ShapeDtypeStruct((n_chunks - 2, n_chunks - 1, 2, HALF, CHUNK), jnp.float32),
            pltpu.VMEM((CORES, ny, nx, n_chunks, 2, HALF, width), gradient.dtype),
            pltpu.VMEM(right_stat.shape, jnp.float32),
            pltpu.VMEM((rows, width), jnp.float32),
        ),
        in_specs=[HBM] * 4,
        out_specs=(HBM, VMEM, VMEM, VMEM),
        scratch_shapes=[
            pltpu.VMEM((2, GROUP, HALF, CHUNK), jnp.float32),
            pltpu.VMEM((GROUP - 1, HALF, CHUNK), jnp.float32),
            pltpu.VMEM(right_root.shape, right_root.dtype),
            pltpu.VMEM((2, rows, BATCH * CHUNK), left_root.dtype),
            pltpu.VMEM((BATCH * CHUNK, width), gradient.dtype),
            dma((4, 2, n_chunks // BATCH)), dma((4, 2)), dma((4, 2, n_chunks)), dma((4, 2)),
            dma((n_chunks,)), dma, dma, dma((2,)), dma((2,)), dma, dma, dma((2,)), dma((3,)),
        ],
        compiler_params=pltpu.CompilerParams(collective_id=0, has_side_effects=True, vmem_limit_bytes=SCOPE),
        cost_estimate=pl.CostEstimate(
            flops=rows * rows * slabs * width, bytes_accessed=4 * rows * rows, transcendentals=0),
        name='gather_products',
    )(*operands)


def left_kernel(left_ref, prod_ref, gath, right_ref, dir_ref, out_ref, right_out_ref, dir_out_ref,
                in_a, in_b, in_p, out_a, out_b, a_sem, b_sem, p_sem, oa_sem, ob_sem, side_sem):
    unit = 2 * CHUNK
    n = left_ref.shape[0] // unit
    total = n * (n + 1) // 2

    def place(i):
        first = lax.rem(i, n)
        second = lax.rem(first + i // n, n)
        return jnp.minimum(first, second), jnp.maximum(first, second)

    side_copies = (pltpu.make_async_copy(right_ref, right_out_ref, side_sem.at[0]),
                   pltpu.make_async_copy(dir_ref, dir_out_ref, side_sem.at[1]))
    slabs = [(c, row, col) for c in range(gath.shape[0]) for row in range(gath.shape[1]) for col in range(gath.shape[2])]

    def window(ref, row, col):
        return ref.at[pl.ds(pl.multiple_of(row * unit, unit), unit), pl.ds(pl.multiple_of(col * unit, unit), unit)]

    def a_in(i, slot):
        low, high = place(i)
        return pltpu.make_async_copy(window(left_ref, low, high), in_a.at[slot], a_sem.at[slot])

    def b_in(i, slot):
        low, high = place(i)
        return pltpu.make_async_copy(window(left_ref, high, low), in_b.at[slot], b_sem.at[slot])

    def p_in(i, slot):
        low, high = place(i)
        return pltpu.make_async_copy(prod_ref.at[pl.ds(high * 2, 2), pl.ds(low * 2, 2)], in_p.at[slot], p_sem.at[slot])

    def a_out(i, slot):
        low, high = place(i)
        return pltpu.make_async_copy(out_a.at[slot], window(out_ref, low, high), oa_sem.at[slot])

    def b_out(i, slot):
        low, high = place(i)
        return pltpu.make_async_copy(out_b.at[slot], window(out_ref, high, low), ob_sem.at[slot])

    def fetch(i):
        slot = lax.rem(i, SLOTS)
        a_in(i, slot).start()

        @pl.when(place(i)[1] < n - 1)
        def _():
            p_in(i, slot).start()

        @pl.when(i >= n)
        def _():
            b_in(i, slot).start()

    for i in range(SLOTS - 1):
        fetch(i)
    for copy in side_copies:
        copy.start()

    def step(i, _):
        slot = lax.rem(i, SLOTS)

        @pl.when(i + SLOTS - 1 < total)
        def _():
            fetch(i + SLOTS - 1)

        low, high = place(i)

        @pl.when(high < n - 1)
        def _():
            p_in(i, slot).wait()

        @pl.when(high == n - 1)
        def _():
            def piece(k, _):
                lhs = jnp.concatenate([gath[c, row, col, pl.ds(low * 2, 2)].reshape(unit, -1) for c, row, col in slabs], axis=1)
                rhs = jnp.concatenate([gath[c, row, col, 2 * n - 2 + k].reshape(CHUNK, -1) for c, row, col in slabs], axis=1)
                out = lax.dot_general(lhs, rhs, NT, preferred_element_type=jnp.float32)
                in_p[slot, k] = out.reshape(2, 2, HALF, CHUNK)
                return 0
            lax.fori_loop(0, 2, piece, 0)

        a_in(i, slot).wait()

        @pl.when(i >= n)
        def _():
            b_in(i, slot).wait()

        @pl.when(i >= SLOTS)
        def _():
            a_out(i, slot).wait()

        @pl.when(i >= n + SLOTS)
        def _():
            b_out(i, slot).wait()

        def part(k, s):
            return in_p[slot, k, s].reshape(CHUNK, CHUNK)

        def mix(stat, prod):
            return EMA_DECAY * stat + (1.0 - EMA_DECAY) * prod

        spans = [slice(0, CHUNK), slice(CHUNK, unit)]

        @pl.when(i < n)
        def _():
            for r in range(2):
                for c in range(2):
                    prod = part(c, r) if c >= r else part(r, c).T
                    out_a[slot, spans[r], spans[c]] = mix(in_a[slot, spans[r], spans[c]], prod)

        @pl.when(i >= n)
        def _():
            for r in range(2):
                for c in range(2):
                    out_a[slot, spans[r], spans[c]] = mix(in_a[slot, spans[r], spans[c]], part(c, r))
                    out_b[slot, spans[c], spans[r]] = mix(in_b[slot, spans[c], spans[r]], part(c, r).T)
            b_out(i, slot).start()
        a_out(i, slot).start()
        return 0

    lax.fori_loop(0, total, step, 0)
    for slot in range(SLOTS):
        a_out(0, slot).wait()
        b_out(0, slot).wait()
    for copy in side_copies:
        copy.wait()


def left_update(left_stat, prod, gath, right_new, direction):
    rows = left_stat.shape[0]
    block = (SLOTS, 2 * CHUNK, 2 * CHUNK)
    kept = [pltpu.with_memory_space_constraint(a, pltpu.VMEM) for a in (gath, right_new, direction)]
    dma = pltpu.SemaphoreType.DMA
    return pl.pallas_call(
        left_kernel,
        out_shape=tuple(jax.ShapeDtypeStruct(a.shape, a.dtype) for a in (left_stat, right_new, direction)),
        in_specs=[HBM, HBM, VMEM, VMEM, VMEM],
        out_specs=(HBM,) * 3,
        scratch_shapes=[
            pltpu.VMEM(block, jnp.float32), pltpu.VMEM(block, jnp.float32),
            pltpu.VMEM((SLOTS, 2, 2, 2, HALF, CHUNK), jnp.float32),
            pltpu.VMEM(block, jnp.float32), pltpu.VMEM(block, jnp.float32),
        ] + [dma((SLOTS,))] * 5 + [dma((2,))],
        compiler_params=pltpu.CompilerParams(vmem_limit_bytes=SCOPE),
        cost_estimate=pl.CostEstimate(flops=4 * rows * rows, bytes_accessed=10 * rows * rows, transcendentals=0),
        name='left_update',
    )(left_stat, prod, *kept)


def solution(mesh):
    stat_spec = P('layer', None)
    shard_spec = P('layer', 'tensor')
    row_spec = P(('layer', 'tensor'), None)

    def local_step(gradient, left_stat, right_stat, left_root, right_root):
        kept = gather_products(mesh, gradient, right_root, right_stat, left_root)
        return left_update(left_stat, *kept)

    return jax.shard_map(local_step, mesh=mesh, in_specs=(shard_spec, stat_spec, row_spec, stat_spec, row_spec), out_specs=(stat_spec, row_spec, shard_spec), check_vma=False)
```

```python
import functools

import jax
import jax.numpy as jnp
from jax import lax
from jax.experimental import pallas as pl
from jax.experimental.pallas import tpu as pltpu
from jax.sharding import PartitionSpec as P

EMA_DECAY = 0.9
CORES = 2
HALF = 128
CHUNK = 2 * HALF
BATCH = 2
GROUP = 4
SLOTS = 4
SCOPE = 57 * 2**19
NT = (((1,), (1,)), ((), ()))
TN = (((0,), (0,)), ((), ()))
HBM = pl.BlockSpec(memory_space=pltpu.HBM)
VMEM = pl.BlockSpec(memory_space=pltpu.VMEM)


def gather_kernel(nx, ny, grad_ref, root_ref, stat_ref, left_root_ref, prod_ref, gath, right_acc, dir_acc,
                  acc, acc_rem, root, left_root, precond,
                  p1_recv, p1_send, p2_recv, p2_send, plane_recv, plane_send, prod_recv, prod_send, prod_local,
                  rem_send, rem_local, lr_sem, misc_sem):
    n_chunks = grad_ref.shape[0]
    n_kept = prod_ref.shape[0]
    n_batches = n_chunks // BATCH
    me = lax.axis_index('tensor')
    core = lax.rem(me, CORES)
    x = lax.rem(me // CORES, nx)
    y = me // (CORES * nx)
    xs = [lax.rem(x + d, nx) for d in range(nx)]
    ys = [lax.rem(y + d, ny) for d in range(ny)]

    def device(row, col, c):
        return {'tensor': (row * nx + col) * CORES + c}

    partner = device(y, x, 1 - core)
    targets = [device(y, xs[1], core), device(y, xs[-1], core), device(ys[1], x, core), device(ys[-1], x, core)]

    def remote(src, target, send, recv, dst=None):
        return pltpu.make_async_remote_copy(
            src_ref=src, dst_ref=src if dst is None else dst, send_sem=send, recv_sem=recv,
            device_id=target, device_id_type=pl.DeviceIdType.MESH)

    def p1_region(direction, hop, batch, back):
        half = direction // 2
        up = direction % 2 == 0
        shift = -back if up else back
        row, col = (y, xs[shift % nx]) if half == 0 else (ys[shift % ny], x)
        if hop == 0:
            span = pl.ds(batch * BATCH, BATCH)
        else:
            span = pl.ds(batch * BATCH + (0 if up else BATCH // 2), BATCH // 2)
        return gath.at[core, row, col, span, half]

    def p1_copy(direction, hop, batch, back):
        return remote(p1_region(direction, hop, batch, back), targets[direction],
                      p1_send.at[direction, hop], p1_recv.at[direction, hop, batch])

    def p2_region(direction, hop, chunk, back):
        half = 1 - direction // 2
        up = direction % 2 == 0
        shift = -back if up else back
        if half == 0:
            span = pl.ds(0, nx) if hop == 0 else pl.ds(0 if up else nx // 2, nx // 2)
            return gath.at[core, ys[shift % ny], span, chunk, half]
        span = pl.ds(0, ny) if hop == 0 else pl.ds(0 if up else ny // 2, ny // 2)
        return gath.at[core, span, xs[shift % nx], chunk, half]

    def p2_copy(direction, hop, chunk, back):
        return remote(p2_region(direction, hop, chunk, back), targets[direction],
                      p2_send.at[direction, hop], p2_recv.at[direction, hop, chunk])

    def plane_copy(chunk, plane):
        return remote(gath.at[plane, :, :, chunk], partner, plane_send, plane_recv.at[chunk])

    def lr_copy(batch):
        slot = lax.rem(batch, 2)
        width = BATCH * CHUNK
        return pltpu.make_async_copy(
            left_root_ref.at[:, pl.ds(pl.multiple_of(batch * width, width), width)], left_root.at[slot], lr_sem.at[slot])

    own_copy = pltpu.make_async_copy(grad_ref, gath.at[core, y, x], misc_sem.at[0])
    root_copy = pltpu.make_async_copy(root_ref, root, misc_sem.at[1])
    stat_copy = pltpu.make_async_copy(stat_ref, right_acc, misc_sem.at[2])
    own_copy.start()
    root_copy.start()
    stat_copy.start()
    lr_copy(0).start()

    barrier = pltpu.get_barrier_semaphore()
    for target in targets + [partner]:
        pl.semaphore_signal(barrier, inc=1, device_id=target, device_id_type=pl.DeviceIdType.MESH)
    pl.semaphore_wait(barrier, len(targets) + 1)

    own_copy.wait()
    lead_in = min(3, n_batches)
    for batch in range(lead_in):
        for direction in range(4):
            p1_copy(direction, 0, batch, 0).start()

    def p1_forward(batch):
        for direction in range(4):
            p1_copy(direction, 0, batch, 1).wait_recv()
        for direction in range(4):
            p1_copy(direction, 1, batch, 1).start()

    for batch in range(lead_in - 1):
        p1_forward(batch)

    root_copy.wait()
    stat_copy.wait()
    right_acc[...] = EMA_DECAY * right_acc[...]
    dir_acc[...] = jnp.zeros_like(dir_acc)

    slabs = [(c, row, col) for c in range(CORES) for row in range(ny) for col in range(nx)]

    def tile(chunk, start, count):
        lhs = jnp.concatenate(
            [gath[c, row, col, pl.ds(start, count), core].reshape(count * HALF, -1) for c, row, col in slabs], axis=1)
        rhs = jnp.concatenate([gath[c, row, col, chunk].reshape(CHUNK, -1) for c, row, col in slabs], axis=1)
        out = lax.dot_general(lhs, rhs, NT, preferred_element_type=jnp.float32)
        return out.reshape(count, HALF, CHUNK)

    def full_out(slot, chunk, start):
        dst = prod_ref.at[chunk, pl.ds(start, GROUP), core]
        return (pltpu.make_async_copy(acc.at[slot], dst, prod_local.at[slot]),
                remote(acc.at[slot], partner, prod_send.at[slot], prod_recv, dst))

    def rem_out(chunk, start, count):
        dst = prod_ref.at[chunk, pl.ds(start, count), core]
        src = acc_rem.at[pl.ds(0, count)]
        return (pltpu.make_async_copy(src, dst, rem_local), remote(src, partner, rem_send, prod_recv, dst))

    def await_out(copies):
        copies[0].wait()
        copies[1].wait_send()

    def side(batch):
        span = pl.ds(batch * BATCH, BATCH)
        block = jnp.concatenate(
            [gath[c, y, col, span].reshape(BATCH * CHUNK, -1) for col in range(nx) for c in range(CORES)], axis=1)
        own = gath[core, y, x, span].reshape(BATCH * CHUNK, -1)
        precond[...] = lax.dot_general(block, root[...], NT, preferred_element_type=jnp.float32).astype(precond.dtype)
        right_acc[...] += (1.0 - EMA_DECAY) * lax.dot_general(own, block, TN, preferred_element_type=jnp.float32)
        slot = lax.rem(batch, 2)
        lr_copy(batch).wait()

        @pl.when(batch + 1 < n_batches)
        def _():
            lr_copy(batch + 1).start()
        band = dir_acc.shape[0] // 4
        for m in range(4):
            rows = slice(m * band, (m + 1) * band)
            dir_acc[rows, :] += jnp.dot(left_root[slot, rows, :], precond[...], preferred_element_type=jnp.float32)

    def full(chunk, g, t):
        slot = lax.rem(t, 2)

        @pl.when(t >= 2)
        def _():
            await_out(full_out(slot, 0, 0))
        acc[slot] = tile(chunk, g * GROUP, GROUP)
        for copy in full_out(slot, chunk, g * GROUP):
            copy.start()
        return t + 1

    def rest(chunk):
        count = (chunk + 1) // GROUP
        left = lax.rem(chunk + 1, GROUP)
        for size in range(1, GROUP):
            before = size - 1 if size > 1 else GROUP - 1

            @pl.when(left == size)
            def _(size=size, before=before):
                @pl.when(chunk >= GROUP if size == 1 else chunk >= 0)
                def _():
                    await_out(rem_out(0, 0, before))
                acc_rem[pl.ds(0, size)] = tile(chunk, count * GROUP, size)
                for copy in rem_out(chunk, count * GROUP, size):
                    copy.start()

    lead = 4

    def step(s, done):
        k = s - lead
        ahead = k + lead

        @pl.when(ahead < n_chunks)
        def _():
            batch = ahead // BATCH

            @pl.when(lax.rem(ahead, BATCH) == 0)
            def _():
                for direction in range(4):
                    p1_copy(direction, 1, batch, 2).wait_recv()
            for direction in range(4):
                p2_copy(direction, 0, ahead, 0).start()

            @pl.when(jnp.logical_and(lax.rem(ahead, BATCH) == 0, batch + lead_in < n_batches))
            def _():
                for direction in range(4):
                    p1_copy(direction, 0, batch + lead_in, 0).start()

            @pl.when(jnp.logical_and(lax.rem(ahead, BATCH) == 1, batch + lead_in - 1 < n_batches))
            def _():
                p1_forward(batch + lead_in - 1)

        @pl.when(jnp.logical_and(k >= 0, k < n_chunks))
        def _():
            for direction in range(4):
                p2_copy(direction, 1, k, 2).wait_recv()
            plane_copy(k, core).start()

        @pl.when(k >= 1)
        def _():
            plane_copy(k - 1, 1 - core).wait_recv()

            @pl.when(lax.rem(k, BATCH) == 0)
            def _():
                side(k // BATCH - 1)

            @pl.when(k - 1 < n_kept)
            def _():
                rest(k - 1)
        count = jnp.where(k - 1 < n_kept, jnp.maximum(k, 0) // GROUP, 0)
        done = lax.fori_loop(0, count // 2, functools.partial(full, k - 1), done)

        @pl.when(jnp.logical_and(k + 2 >= 0, k + 2 < n_chunks))
        def _():
            for direction in range(4):
                p2_copy(direction, 0, k + 2, 1).wait_recv()
            for direction in range(4):
                p2_copy(direction, 1, k + 2, 1).start()
        return lax.fori_loop(count // 2, count, functools.partial(full, k - 1), done)

    lax.fori_loop(0, n_chunks + lead + 1, step, 0)

    for slot in range(2):
        await_out(full_out(slot, 0, 0))
    await_out(rem_out(0, 0, n_kept % GROUP))
    tiles = prod_ref.at[pl.ds(0, n_kept // 2), :, 0]
    remote(tiles, partner, prod_send.at[0], prod_recv).wait_recv()
    for direction in range(4):
        half = direction // 2
        remote(gath.at[core, y, x, :, half], partner, p1_send.at[direction, 0], p1_recv.at[0, 0, 0]).wait_send()
        remote(gath.at[core, y, x, pl.ds(0, n_chunks // 2), half], partner, p1_send.at[direction, 1], p1_recv.at[0, 0, 0]).wait_send()
        remote(gath.at[core, y, :, :, 0], partner, p2_send.at[direction, 0], p1_recv.at[0, 0, 0]).wait_send()
        remote(gath.at[core, y, pl.ds(0, nx // 2), :, 0], partner, p2_send.at[direction, 1], p1_recv.at[0, 0, 0]).wait_send()
    remote(gath.at[core], partner, plane_send, p1_recv.at[0, 0, 0]).wait_send()


def gather_products(mesh, gradient, right_root, right_stat, left_root):
    rows, width = gradient.shape
    n_chunks = rows // CHUNK
    n_devices = mesh.shape['tensor']
    group = right_stat.shape[1] // width
    nx, ny = group // CORES, n_devices // group
    dma = pltpu.SemaphoreType.DMA
    slabs = n_devices
    operands = [pltpu.with_memory_space_constraint(a, pltpu.HBM) for a in (
        gradient.reshape(n_chunks, 2, HALF, width), right_root, right_stat, left_root)]
    return pl.pallas_call(
        functools.partial(gather_kernel, nx, ny),
        out_shape=(
            jax.ShapeDtypeStruct((n_chunks - 2, n_chunks - 1, 2, HALF, CHUNK), jnp.float32),
            pltpu.VMEM((CORES, ny, nx, n_chunks, 2, HALF, width), gradient.dtype),
            pltpu.VMEM(right_stat.shape, jnp.float32),
            pltpu.VMEM((rows, width), jnp.float32),
        ),
        in_specs=[HBM] * 4,
        out_specs=(HBM, VMEM, VMEM, VMEM),
        scratch_shapes=[
            pltpu.VMEM((2, GROUP, HALF, CHUNK), jnp.float32),
            pltpu.VMEM((GROUP - 1, HALF, CHUNK), jnp.float32),
            pltpu.VMEM(right_root.shape, right_root.dtype),
            pltpu.VMEM((2, rows, BATCH * CHUNK), left_root.dtype),
            pltpu.VMEM((BATCH * CHUNK, width), gradient.dtype),
            dma((4, 2, n_chunks // BATCH)), dma((4, 2)), dma((4, 2, n_chunks)), dma((4, 2)),
            dma((n_chunks,)), dma, dma, dma((2,)), dma((2,)), dma, dma, dma((2,)), dma((3,)),
        ],
        compiler_params=pltpu.CompilerParams(collective_id=0, has_side_effects=True, vmem_limit_bytes=SCOPE),
        cost_estimate=pl.CostEstimate(
            flops=rows * rows * slabs * width, bytes_accessed=4 * rows * rows, transcendentals=0),
        name='gather_products',
    )(*operands)


def left_kernel(left_ref, prod_ref, gath, right_ref, dir_ref, out_ref, right_out_ref, dir_out_ref,
                in_a, in_b, in_p, out_a, out_b, a_sem, b_sem, p_sem, oa_sem, ob_sem, side_sem):
    unit = 2 * CHUNK
    n = left_ref.shape[0] // unit
    total = n * (n + 1) // 2

    def place(i):
        first = lax.rem(i, n)
        second = lax.rem(first + i // n, n)
        first, second = lax.rem(first + n - 1, n), lax.rem(second + n - 1, n)
        return jnp.minimum(first, second), jnp.maximum(first, second)

    side_copies = (pltpu.make_async_copy(right_ref, right_out_ref, side_sem.at[0]),
                   pltpu.make_async_copy(dir_ref, dir_out_ref, side_sem.at[1]))
    slabs = [(c, row, col) for c in range(gath.shape[0]) for row in range(gath.shape[1]) for col in range(gath.shape[2])]

    def window(ref, row, col):
        return ref.at[pl.ds(pl.multiple_of(row * unit, unit), unit), pl.ds(pl.multiple_of(col * unit, unit), unit)]

    def a_in(i, slot):
        low, high = place(i)
        return pltpu.make_async_copy(window(left_ref, low, high), in_a.at[slot], a_sem.at[slot])

    def b_in(i, slot):
        low, high = place(i)
        return pltpu.make_async_copy(window(left_ref, high, low), in_b.at[slot], b_sem.at[slot])

    def p_in(i, slot):
        low, high = place(i)
        return pltpu.make_async_copy(prod_ref.at[pl.ds(high * 2, 2), pl.ds(low * 2, 2)], in_p.at[slot], p_sem.at[slot])

    def a_out(i, slot):
        low, high = place(i)
        return pltpu.make_async_copy(out_a.at[slot], window(out_ref, low, high), oa_sem.at[slot])

    def b_out(i, slot):
        low, high = place(i)
        return pltpu.make_async_copy(out_b.at[slot], window(out_ref, high, low), ob_sem.at[slot])

    def fetch(i):
        slot = lax.rem(i, SLOTS)
        a_in(i, slot).start()

        @pl.when(place(i)[1] < n - 1)
        def _():
            p_in(i, slot).start()

        @pl.when(i >= n)
        def _():
            b_in(i, slot).start()

    for i in range(SLOTS - 1):
        fetch(i)
    for copy in side_copies:
        copy.start()

    def step(i, _):
        slot = lax.rem(i, SLOTS)

        @pl.when(i + SLOTS - 1 < total)
        def _():
            fetch(i + SLOTS - 1)

        low, high = place(i)

        @pl.when(high < n - 1)
        def _():
            p_in(i, slot).wait()

        @pl.when(high == n - 1)
        def _():
            def piece(k, _):
                lhs = jnp.concatenate([gath[c, row, col, pl.ds(low * 2, 2)].reshape(unit, -1) for c, row, col in slabs], axis=1)
                rhs = jnp.concatenate([gath[c, row, col, 2 * n - 2 + k].reshape(CHUNK, -1) for c, row, col in slabs], axis=1)
                out = lax.dot_general(lhs, rhs, NT, preferred_element_type=jnp.float32)
                in_p[slot, k] = out.reshape(2, 2, HALF, CHUNK)
                return 0
            lax.fori_loop(0, 2, piece, 0)

        a_in(i, slot).wait()

        @pl.when(i >= n)
        def _():
            b_in(i, slot).wait()

        @pl.when(i >= SLOTS)
        def _():
            a_out(i, slot).wait()

        @pl.when(i >= n + SLOTS)
        def _():
            b_out(i, slot).wait()

        def part(k, s):
            return in_p[slot, k, s].reshape(CHUNK, CHUNK)

        def mix(stat, prod):
            return EMA_DECAY * stat + (1.0 - EMA_DECAY) * prod

        spans = [slice(0, CHUNK), slice(CHUNK, unit)]

        @pl.when(i < n)
        def _():
            for r in range(2):
                for c in range(2):
                    prod = part(c, r) if c >= r else part(r, c).T
                    out_a[slot, spans[r], spans[c]] = mix(in_a[slot, spans[r], spans[c]], prod)

        @pl.when(i >= n)
        def _():
            for r in range(2):
                for c in range(2):
                    out_a[slot, spans[r], spans[c]] = mix(in_a[slot, spans[r], spans[c]], part(c, r))
                    out_b[slot, spans[c], spans[r]] = mix(in_b[slot, spans[c], spans[r]], part(c, r).T)
            b_out(i, slot).start()
        a_out(i, slot).start()
        return 0

    lax.fori_loop(0, total, step, 0)
    for slot in range(SLOTS):
        a_out(0, slot).wait()
        b_out(0, slot).wait()
    for copy in side_copies:
        copy.wait()


def left_update(left_stat, prod, gath, right_new, direction):
    rows = left_stat.shape[0]
    block = (SLOTS, 2 * CHUNK, 2 * CHUNK)
    kept = [pltpu.with_memory_space_constraint(a, pltpu.VMEM) for a in (gath, right_new, direction)]
    dma = pltpu.SemaphoreType.DMA
    return pl.pallas_call(
        left_kernel,
        out_shape=tuple(jax.ShapeDtypeStruct(a.shape, a.dtype) for a in (left_stat, right_new, direction)),
        in_specs=[HBM, HBM, VMEM, VMEM, VMEM],
        out_specs=(HBM,) * 3,
        scratch_shapes=[
            pltpu.VMEM(block, jnp.float32), pltpu.VMEM(block, jnp.float32),
            pltpu.VMEM((SLOTS, 2, 2, 2, HALF, CHUNK), jnp.float32),
            pltpu.VMEM(block, jnp.float32), pltpu.VMEM(block, jnp.float32),
        ] + [dma((SLOTS,))] * 5 + [dma((2,))],
        compiler_params=pltpu.CompilerParams(vmem_limit_bytes=SCOPE),
        cost_estimate=pl.CostEstimate(flops=4 * rows * rows, bytes_accessed=10 * rows * rows, transcendentals=0),
        name='left_update',
    )(left_stat, prod, *kept)


def solution(mesh):
    stat_spec = P('layer', None)
    shard_spec = P('layer', 'tensor')
    row_spec = P(('layer', 'tensor'), None)

    def local_step(gradient, left_stat, right_stat, left_root, right_root):
        kept = gather_products(mesh, gradient, right_root, right_stat, left_root)
        return left_update(left_stat, *kept)

    return jax.shard_map(local_step, mesh=mesh, in_specs=(shard_spec, stat_spec, row_spec, stat_spec, row_spec), out_specs=(stat_spec, row_spec, shard_spec), check_vma=False)
```
